32 devices in a mesh: dp: 1 (over z), col: 4 (over y), row: 8 (over x, core).
Axes of the slice: x: 4, y: 4, z: 1, core: 2. Of those that a mesh axis runs over, the one named last changes fastest.
The devices are a block of a 4x4x8 slice.
Arguments:
- latent: bfloat16 [4, 16, 384, 640], P('dp', 'row', 'col')
- t_emb: bfloat16 [4, 1280], P('dp')
- res_norm: bfloat16 [2, 2, 2, 640], replicated
- res_conv: bfloat16 [2, 2, 3, 3, 640, 640], replicated
- res_temb: bfloat16 [2, 1280, 640], replicated
- attn_norm: bfloat16 [2, 640], replicated
- attn_proj: bfloat16 [4, 10, 640, 64], replicated
Outputs:
- output: bfloat16 [4, 16, 384, 640], P('dp', 'row', 'col')
All inputs are finite; a program needn't handle non-finite values.
Results may differ from the reference program's by a relative error of at most 0.0114891.
Values are sent between devices in bfloat16 or wider.
A program may use at most 768 MiB of HBM per device.

```python
import jax
import jax.numpy as jnp
from jax import lax

BATCH = 4
HEIGHT = 16
WIDTH = 384
CHANNELS = 640
HEADS = 10
TEMB_DIM = 1280
GROUPS = 32
Q_BLOCK = 192
EPS = 1e-5
HEAD_DIM = CHANNELS // HEADS


def setup_inputs(seed: int = 0, part: int = 0) -> dict:
    part_keys = jax.random.split(jax.random.fold_in(jax.random.key(seed), part), 3)
    shared_keys = jax.random.split(jax.random.key(seed + 1), 5)
    base_noise = jax.random.normal(part_keys[0], (BATCH, HEIGHT, WIDTH, CHANNELS), jnp.float32)
    slopes = 1.5 * jax.random.normal(part_keys[1], (2, BATCH, 1, 1, CHANNELS), jnp.float32)
    ramp_rows = jnp.linspace(-1.0, 1.0, HEIGHT)[None, :, None, None]
    ramp_cols = jnp.linspace(-1.0, 1.0, WIDTH)[None, None, :, None]
    latent = base_noise + slopes[0] * ramp_rows + slopes[1] * ramp_cols
    t_emb = jax.random.normal(part_keys[2], (BATCH, TEMB_DIM), jnp.float32)
    norm_draw = jax.random.normal(shared_keys[0], (2, 2, 2, CHANNELS), jnp.float32)
    res_norm = jnp.stack([1.0 + 0.3 * norm_draw[:, :, 0], 0.5 * norm_draw[:, :, 1]], axis=2)
    res_conv = jax.random.normal(shared_keys[1], (2, 2, 3, 3, CHANNELS, CHANNELS), jnp.float32) * (9 * CHANNELS) ** -0.5
    res_temb = jax.random.normal(shared_keys[2], (2, TEMB_DIM, CHANNELS), jnp.float32) * TEMB_DIM ** -0.5
    attn_draw = jax.random.normal(shared_keys[3], (2, CHANNELS), jnp.float32)
    attn_norm = jnp.stack([1.0 + 0.3 * attn_draw[0], 0.5 * attn_draw[1]])
    proj_gain = jnp.array([1.5, 1.5, 1.0, 1.5], jnp.float32)[:, None, None, None]
    attn_proj = jax.random.normal(shared_keys[4], (4, HEADS, CHANNELS, HEAD_DIM), jnp.float32) * proj_gain * CHANNELS ** -0.5
    return {
        'latent': latent.astype(jnp.bfloat16),
        't_emb': t_emb.astype(jnp.bfloat16),
        'res_norm': res_norm.astype(jnp.bfloat16),
        'res_conv': res_conv.astype(jnp.bfloat16),
        'res_temb': res_temb.astype(jnp.bfloat16),
        'attn_norm': attn_norm.astype(jnp.bfloat16),
        'attn_proj': attn_proj.astype(jnp.bfloat16),
    }


def group_norm(values, gn_scale, gn_shift):
    group_ch = CHANNELS // GROUPS
    grouped = values.astype(jnp.float32).reshape(BATCH, HEIGHT, WIDTH, GROUPS, group_ch)
    elem_count = HEIGHT * WIDTH * group_ch
    mean_val = jnp.sum(grouped, axis=(1, 2, 4)) / elem_count
    mean_sq = jnp.sum(grouped * grouped, axis=(1, 2, 4)) / elem_count
    inv_std = lax.rsqrt(mean_sq - mean_val * mean_val + EPS)
    normed = (grouped - mean_val[:, None, None, :, None]) * inv_std[:, None, None, :, None]
    return normed.reshape(values.shape) * gn_scale.astype(jnp.float32) + gn_shift.astype(jnp.float32)


def conv3x3(acts_in, kernel):
    return lax.conv_general_dilated(acts_in.astype(jnp.float32), kernel.astype(jnp.float32), (1, 1), ((1, 1), (1, 1)), dimension_numbers=('NHWC', 'HWIO', 'NHWC'))


def res_block(latent, t_emb, norm_par, kernels, w_temb):
    t_act = jax.nn.silu(t_emb.astype(jnp.float32)).astype(jnp.bfloat16)
    t_proj = jnp.dot(t_act, w_temb, preferred_element_type=jnp.float32)
    first_act = jax.nn.silu(group_norm(latent, norm_par[0, 0], norm_par[0, 1])).astype(jnp.bfloat16)
    hidden = (conv3x3(first_act, kernels[0]) + t_proj[:, None, None, :]).astype(jnp.bfloat16)
    second_act = jax.nn.silu(group_norm(hidden, norm_par[1, 0], norm_par[1, 1])).astype(jnp.bfloat16)
    return (latent.astype(jnp.float32) + conv3x3(second_act, kernels[1])).astype(jnp.bfloat16)


def attn_block(latent, norm_par, proj_w):
    n_tok = HEIGHT * WIDTH
    normed = group_norm(latent, norm_par[0], norm_par[1]).astype(jnp.bfloat16).reshape(BATCH, n_tok, CHANNELS)
    qkv_all = jnp.einsum('bnc,khcd->kbnhd', normed.astype(jnp.float32), proj_w[:3].astype(jnp.float32)).astype(jnp.bfloat16)
    q_blocks = qkv_all[0].reshape(BATCH, n_tok // Q_BLOCK, Q_BLOCK, HEADS, HEAD_DIM)
    k_all = qkv_all[1].astype(jnp.float32)
    v_all = qkv_all[2].astype(jnp.float32)

    def one_image(image_args):
        q_img, k_img, v_img = image_args

        def one_block(q_blk):
            logits = jnp.einsum('qhd,khd->hqk', q_blk.astype(jnp.float32), k_img) * HEAD_DIM ** -0.5
            att_weights = jax.nn.softmax(logits, axis=-1)
            return jnp.einsum('hqk,khd->qhd', att_weights, v_img)

        return lax.map(one_block, q_img)

    attn_out = lax.map(one_image, (q_blocks, k_all, v_all)).reshape(BATCH, n_tok, HEADS, HEAD_DIM)
    out_proj = jnp.einsum('bnhd,hcd->bnc', attn_out.astype(jnp.bfloat16).astype(jnp.float32), proj_w[3].astype(jnp.float32))
    return (latent.astype(jnp.float32) + out_proj.reshape(latent.shape)).astype(jnp.bfloat16)


def reference(latent, t_emb, res_norm, res_conv, res_temb, attn_norm, attn_proj):
    hidden = res_block(latent, t_emb, res_norm[0], res_conv[0], res_temb[0])
    hidden = attn_block(hidden, attn_norm, attn_proj)
    return res_block(hidden, t_emb, res_norm[1], res_conv[1], res_temb[1])
```

```python
import functools

import jax
import jax.numpy as jnp
import numpy as np
from jax import lax
from jax.experimental import pallas as pl
from jax.experimental.pallas import tpu as pltpu
from jax.sharding import PartitionSpec as P

GROUPS = 32
EPS = 1e-5
F32 = jnp.float32
BF16 = jnp.bfloat16
LOG2E = 1.4426950408889634
KEY_BLK = 512


class Place:
    def __init__(self, dims):
        self.n_img, self.n_row, self.n_col, self.rows, self.cols, self.chan = dims
        self.halves = self.n_row // self.n_img
        self.seg = self.n_row // self.halves
        self.row = lax.axis_index('row')
        self.col = lax.axis_index('col')
        self.img = self.row // self.halves
        self.half = self.row % self.halves
        self.n_peer = self.halves * self.n_col
        self.me = self.half * self.n_col + self.col

    def peer(self, step):
        slot = (self.me + step) % self.n_peer
        return {'row': self.img * self.halves + slot // self.n_col, 'col': slot % self.n_col}

    def partner(self):
        return {'row': self.img * self.halves + (1 - self.half), 'col': self.col}

    def beside(self, step, other=False):
        half = (1 - self.half) if other else self.half
        return {'row': self.img * self.halves + half, 'col': (self.col + step + self.n_col) % self.n_col}


def remote(src, dst, send_sem, recv_sem, device):
    return pltpu.make_async_remote_copy(src_ref=src, dst_ref=dst, send_sem=send_sem, recv_sem=recv_sem, device_id=device, device_id_type=pl.DeviceIdType.MESH)


def signal_peers(at, with_column):
    barrier = pltpu.get_barrier_semaphore()
    for step in range(1, at.n_peer):
        pl.semaphore_signal(barrier, inc=1, device_id=at.peer(step), device_id_type=pl.DeviceIdType.MESH)
    count = at.n_peer - 1
    if with_column:
        for step in range(1, at.n_img):
            for half in range(at.halves):
                row = ((at.img + step) % at.n_img) * at.halves + half
                pl.semaphore_signal(barrier, inc=1, device_id={'row': row, 'col': at.col}, device_id_type=pl.DeviceIdType.MESH)
                count += 1
    return count


def wait_peers(count):
    pl.semaphore_wait(pltpu.get_barrier_semaphore(), count)


def stat_copies(at, mine, every, ssem, rsem):
    out = []
    for step in range(1, at.n_peer):
        send = remote(mine, every.at[at.me], ssem.at[step - 1], rsem.at[step - 1], at.peer(step))
        source = (at.me - step + at.n_peer) % at.n_peer
        recv = remote(mine, every.at[source], ssem.at[step - 1], rsem.at[step - 1], at.peer(step))
        out.append((send, recv))
    return out


def halo_copies(at, full, hrow, colbuf, hcol, ssem, rsem):
    base = at.n_peer - 1
    edge = (at.rows * at.seg - 1) * (1 - at.half)
    out = []
    copy = remote(full.at[edge], hrow, ssem.at[base], rsem.at[base], at.partner())
    out.append((copy, copy))
    for slot, (side, step, other) in enumerate([(1, 1, False), (1, 1, True), (0, -1, False), (0, -1, True)]):
        copy = remote(colbuf.at[side], hcol.at[slot], ssem.at[base + 1 + slot], rsem.at[base + 1 + slot], at.beside(step, other))
        out.append((copy, copy))
    return out


def put_stats(stats, mine, every, at):
    s1 = jnp.sum(stats[0], axis=0, keepdims=True)
    s2 = jnp.sum(stats[1], axis=0, keepdims=True)
    idx = lax.broadcasted_iota(jnp.int32, mine.shape, 0)
    both = jnp.where(idx == 0, s1, jnp.where(idx == 1, s2, 0.0))
    mine[...] = both
    every[at.me] = both


def swap_all(at, mine, every, ssem, rsem, full=None, hrow=None, colbuf=None, hcol=None):
    copies = [] if full is None else halo_copies(at, full, hrow, colbuf, hcol, ssem, rsem)
    copies += stat_copies(at, mine, every, ssem, rsem)
    for send, _ in copies:
        send.start()
    for _, recv in copies:
        recv.wait_recv()
    for send, _ in copies:
        send.wait_send()


def norm_terms(every, member, scale, shift, count):
    total = every[0]
    for slot in range(1, every.shape[0]):
        total = total + every[slot]
    high = total.astype(BF16).astype(F32)
    mid = (total - high).astype(BF16).astype(F32)
    low = (total - high - mid).astype(BF16).astype(F32)
    stacked = jnp.concatenate([high, mid, low, jnp.zeros_like(low)], axis=0).astype(BF16)
    n = total.shape[0]
    summed = jnp.dot(stacked, member[...], preferred_element_type=F32)
    sums = summed[0:n] + summed[n:2 * n] + summed[2 * n:3 * n]
    mean = sums[0:1] / count
    var = sums[1:2] / count - mean * mean
    return mean, lax.rsqrt(var + EPS) * scale, shift


def activate(x, terms):
    mean, scale, shift = terms
    u = (x - mean) * scale + shift
    return u / (1.0 + jnp.exp(-u))


def add_stats(stats, vals):
    n, chan = vals.shape
    split = vals.reshape(n // 8, 8, chan)
    return stats[0] + jnp.sum(split, axis=0), stats[1] + jnp.sum(split * split, axis=0)


def zero_stats(chan):
    return jnp.zeros((8, chan), F32), jnp.zeros((8, chan), F32)


def keep_cols(colbuf, first_row, vals, n_rows, cols):
    for k in range(n_rows):
        colbuf[0, pl.ds(first_row + k, 1), :] = vals[k * cols:k * cols + 1]
        colbuf[1, pl.ds(first_row + k, 1), :] = vals[(k + 1) * cols - 1:(k + 1) * cols]


def fill_taps(at, full, hrow, hcol, terms, taps, colact):
    chan, cols = at.chan, at.cols
    n_own = at.rows * at.seg
    for slot in range(4):
        inside = (at.col > 0) if slot < 2 else (at.col < at.n_col - 1)
        colact[slot] = jnp.where(inside, activate(hcol[slot], terms), 0.0)
    row_id = lax.broadcasted_iota(jnp.int32, (cols, chan), 0)

    def put(dst, x, left, right):
        act = activate(x.astype(F32), terms)
        prev = jnp.where(row_id == 0, left, pltpu.roll(act, 1, 0))
        nxt = jnp.where(row_id == cols - 1, right, pltpu.roll(act, cols - 1, 0))
        taps[dst, :, 0:chan] = prev.astype(BF16)
        taps[dst, :, chan:2 * chan] = act.astype(BF16)
        taps[dst, :, 2 * chan:3 * chan] = nxt.astype(BF16)

    def own(r, _):
        put(r + 1, full[r], colact[0, pl.ds(r, 1), :], colact[2, pl.ds(r, 1), :])
        return 0

    lax.fori_loop(0, n_own, own, 0)
    near = (n_own - 1) * at.half
    put((n_own + 1) * (1 - at.half), hrow[...], colact[1, pl.ds(near, 1), :], colact[3, pl.ds(near, 1), :])
    taps[(n_own + 1) * at.half] = jnp.zeros((cols, 3 * chan), BF16)


def conv_rows(at, taps, weights, first):
    acc = None
    for dy in range(3):
        lhs = taps[pl.ds(first + dy, at.rows)].reshape(at.rows * at.cols, 3 * at.chan)
        part = jnp.dot(lhs, weights[dy].reshape(3 * at.chan, at.chan), preferred_element_type=F32)
        acc = part if acc is None else acc + part
    return acc


def norm_rows(ref):
    vals = ref[...].astype(F32)
    return vals[0:1], vals[1:2]


def res_first(dims, count, blk, latent, temb, norms, w_all, member, x_out, stat_out, xin, hid, taps, wbuf, mine, every, hrow, colbuf, hcol, colact, wsem, ssem, rsem, xs, xr, lsem):
    at = Place(dims)
    n_wait = signal_peers(at, True)
    loads = [pltpu.make_async_copy(w_all.at[blk, j], wbuf.at[j], wsem.at[j]) for j in range(2)]
    for load in loads:
        load.start()
    wait_peers(n_wait)
    target_half, slot = at.row // at.seg, at.row % at.seg
    rows, cols, chan = at.rows, at.cols, at.chan
    for i in range(at.n_img):
        row = i * at.halves + target_half
        dst = xin.at[pl.ds(slot * rows, rows)]

        @pl.when(row == at.row)
        def _():
            pltpu.make_async_copy(latent.at[i], dst, lsem).start()

        @pl.when(row != at.row)
        def _():
            remote(latent.at[i], dst, xs.at[i], xr.at[slot], {'row': row, 'col': at.col}).start()

    stats = zero_stats(chan)
    for k in range(at.seg):
        row = at.half * at.seg + k
        dst = xin.at[pl.ds(k * rows, rows)]

        @pl.when(row == at.row)
        def _():
            pltpu.make_async_copy(latent.at[0], dst, lsem).wait()

        @pl.when(row != at.row)
        def _():
            remote(latent.at[0], dst, xs.at[0], xr.at[k], {'row': row, 'col': at.col}).wait_recv()

        vals = xin[k * rows:(k + 1) * rows].astype(F32).reshape(rows * cols, chan)
        stats = add_stats(stats, vals)
        keep_cols(colbuf.at[0], k * rows, vals, rows, cols)
    put_stats(stats, mine.at[0], every.at[0], at)
    swap_all(at, mine.at[0], every.at[0], ssem.at[0], rsem.at[0], xin, hrow.at[0], colbuf.at[0], hcol.at[0])
    for i in range(at.n_img):
        row = i * at.halves + target_half

        @pl.when(row != at.row)
        def _():
            remote(latent.at[i], xin.at[pl.ds(slot * rows, rows)], xs.at[i], xr.at[slot], {'row': row, 'col': at.col}).wait_send()

    conv_pair(at, count, blk, temb, norms, member, xin, hid, taps, wbuf, mine, every, hrow, colbuf, hcol, colact, loads, ssem, rsem)

    def second(m, stats):
        acc = conv_rows(at, taps, wbuf.at[1], m * rows)
        y = (xin[pl.ds(m * rows, rows)].astype(F32).reshape(rows * cols, chan) + acc).astype(BF16)
        x_out[pl.ds(m * rows, rows)] = y.reshape(rows, cols, chan)
        return add_stats(stats, y.astype(F32))

    stats = lax.fori_loop(0, at.seg, second, zero_stats(chan))
    put_stats(stats, mine.at[2], every.at[2], at)
    swap_all(at, mine.at[2], every.at[2], ssem.at[2], rsem.at[2])
    stat_out[...] = every[2]


def conv_pair(at, count, blk, temb, norms, member, xin, hid, taps, wbuf, mine, every, hrow, colbuf, hcol, colact, loads, ssem, rsem):
    rows, cols, chan = at.rows, at.cols, at.chan
    terms = norm_terms(every.at[0], member, *norm_rows(norms.at[blk, 0]), count)
    fill_taps(at, xin, hrow.at[0], hcol.at[0], terms, taps, colact)
    loads[0].wait()
    shift = temb[blk, pl.ds(at.img, 1), :]

    def first(m, stats):
        h = (conv_rows(at, taps, wbuf.at[0], m * rows) + shift).astype(BF16)
        hid[pl.ds(m * rows, rows)] = h.reshape(rows, cols, chan)
        vals = h.astype(F32)
        keep_cols(colbuf.at[1], m * rows, vals, rows, cols)
        return add_stats(stats, vals)

    stats = lax.fori_loop(0, at.seg, first, zero_stats(chan))
    put_stats(stats, mine.at[1], every.at[1], at)
    swap_all(at, mine.at[1], every.at[1], ssem.at[1], rsem.at[1], hid, hrow.at[1], colbuf.at[1], hcol.at[1])
    terms = norm_terms(every.at[1], member, *norm_rows(norms.at[blk, 1]), count)
    fill_taps(at, hid, hrow.at[1], hcol.at[1], terms, taps, colact)
    loads[1].wait()


def nt(a, b):
    return lax.dot_general(a, b, (((1,), (1,)), ((), ())), preferred_element_type=F32)


def attention(dims, count, x, every, norms, proj, member, out, xall, qm, kbuf, vbuf, sbuf, run_max, run_sum, run_out, ssem, rsem, lsem):
    at = Place(dims)
    n_wait = signal_peers(at, False)
    tok, chan = x.shape
    n_head = qm.shape[0]
    dim = chan // n_head
    half_tok = tok // 2
    own_copy = pltpu.make_async_copy(x, xall.at[0], lsem)
    own_copy.start()
    terms = norm_terms(every, member, *norm_rows(norms), count)

    def normed(vals):
        return ((vals.astype(F32) - terms[0]) * terms[1] + terms[2]).astype(BF16)

    right, left, mate = at.beside(1), at.beside(-1), at.partner()
    low, high = pl.ds(0, half_tok), pl.ds(half_tok, half_tok)

    def link(k, src, slot, device):
        return remote(src, slot, ssem.at[k], rsem.at[k], device)

    to_mate = link(0, x, xall.at[1], mate)
    to_right = link(1, x, xall.at[2], right)
    to_left = link(2, x, xall.at[3], left)
    left_mate = link(3, xall.at[2], xall.at[4], mate)
    right_mate = link(4, xall.at[3], xall.at[5], mate)
    left_right = link(5, xall.at[2, low], xall.at[6, low], right)
    right_left = link(6, xall.at[3, high], xall.at[6, high], left)
    far_low = link(7, xall.at[6, low], xall.at[7, low], mate)
    far_high = link(8, xall.at[6, high], xall.at[7, high], mate)
    wait_peers(n_wait)
    to_right.start()
    to_left.start()
    to_mate.start()

    g = normed(x[...])
    qt = nt(proj[0], g).astype(BF16)
    zero = jnp.zeros((dim, tok), BF16)
    for h in range(n_head):
        mine = (h % 2) * dim
        qm[h, mine:mine + dim, :] = qt[h * dim:(h + 1) * dim]
        qm[h, dim - mine:2 * dim - mine, :] = zero
    run_max[...] = jnp.full(run_max.shape, -1e30, F32)
    run_sum[...] = jnp.zeros(run_sum.shape, F32)
    run_out[...] = jnp.zeros(run_out.shape, F32)
    own_copy.wait()

    factor = LOG2E * dim ** -0.5
    n_blk = 2 * tok // KEY_BLK

    def scores(h, j):
        keys = kbuf[pl.ds(j * KEY_BLK, KEY_BLK), pl.ds(pl.multiple_of((h // 2) * 2 * dim, 2 * dim), 2 * dim)]
        return jnp.dot(keys, qm[h], preferred_element_type=F32)

    def phase(k):
        def project(b, _):
            g = normed(xall[2 * k + b])
            span = pl.ds(pl.multiple_of(b * tok, tok), tok)
            kbuf[span, :] = nt(g, proj[1]).astype(BF16)
            vbuf[:, span] = nt(proj[2], g).astype(BF16)
            return 0

        lax.fori_loop(0, 2, project, 0)
        sbuf[0] = scores(0, 0)

        def pair(p, _):
            for u in range(2 * n_blk):
                h, j = 2 * p + u // n_blk, u % n_blk
                if u + 1 < 2 * n_blk:
                    sbuf[(u + 1) % 2] = scores(2 * p + (u + 1) // n_blk, (u + 1) % n_blk)
                else:
                    sbuf[(u + 1) % 2] = scores(jnp.minimum(2 * p + 2, n_head - 1), 0)
                if j == 0:
                    m, l, acc = run_max[h, 0:1], run_sum[h, 0:1], run_out[h]
                s = sbuf[u % 2]
                new = jnp.maximum(m, jnp.max(s, axis=0, keepdims=True) * factor)
                alpha = jnp.exp2(m - new)
                w = jnp.exp2(s * factor - new)
                l = l * alpha + jnp.sum(w, axis=0, keepdims=True)
                vt = vbuf[pl.ds(pl.multiple_of(h * dim, dim), dim), j * KEY_BLK:(j + 1) * KEY_BLK]
                acc = acc * alpha + jnp.dot(vt, w.astype(BF16), preferred_element_type=F32)
                m = new
                if j == n_blk - 1:
                    run_max[h, 0:1], run_sum[h, 0:1], run_out[h] = m, l, acc
            return 0

        lax.fori_loop(0, n_head // 2, pair, 0)

    def at_phase(k, _):
        @pl.when(k == 0)
        def _():
            to_mate.wait_recv()

        @pl.when(k == 1)
        def _():
            to_right.wait_recv()
            left_right.start()
            left_mate.start()
            to_left.wait_recv()
            right_left.start()
            right_mate.start()

        @pl.when(k == 2)
        def _():
            left_mate.wait_recv()
            right_mate.wait_recv()
            left_right.wait_recv()
            far_low.start()
            right_left.wait_recv()
            far_high.start()

        @pl.when(k == 3)
        def _():
            far_low.wait_recv()
            far_high.wait_recv()

        phase(k)
        return 0

    lax.fori_loop(0, 4, at_phase, 0)
    for copy in (to_mate, to_right, to_left, left_mate, right_mate, left_right, right_left, far_low, far_high):
        copy.wait_send()

    def finish(h, _):
        out[pl.ds(pl.multiple_of(h * dim, dim), dim), :] = (run_out[h] / run_sum[h, 0:1]).astype(BF16)
        return 0

    lax.fori_loop(0, n_head, finish, 0)


def res_second(dims, count, blk, x, ot, proj, temb, norms, w_all, member, y_out, xin, hid, taps, wbuf, mine, every, hrow, colbuf, hcol, colact, ybuf, wsem, ssem, rsem, xs, xr, lsem):
    at = Place(dims)
    n_wait = signal_peers(at, True)
    loads = [pltpu.make_async_copy(w_all.at[blk, j], wbuf.at[j], wsem.at[j]) for j in range(2)]
    for load in loads:
        load.start()
    rows, cols, chan = at.rows, at.cols, at.chan
    tile = rows * cols
    add = lax.dot_general(ot[...], proj[...], (((0,), (0,)), ((), ())), preferred_element_type=F32)
    stats = zero_stats(chan)
    for m in range(at.seg):
        y = (x[m * rows:(m + 1) * rows].astype(F32).reshape(tile, chan) + add[m * tile:(m + 1) * tile]).astype(BF16)
        xin[m * rows:(m + 1) * rows] = y.reshape(rows, cols, chan)
        vals = y.astype(F32)
        stats = add_stats(stats, vals)
        keep_cols(colbuf.at[0], m * rows, vals, rows, cols)
    put_stats(stats, mine.at[0], every.at[0], at)
    wait_peers(n_wait)
    swap_all(at, mine.at[0], every.at[0], ssem.at[0], rsem.at[0], xin, hrow.at[0], colbuf.at[0], hcol.at[0])
    conv_pair(at, count, blk, temb, norms, member, xin, hid, taps, wbuf, mine, every, hrow, colbuf, hcol, colact, loads, ssem, rsem)

    def back(m):
        row = at.half * at.seg + m
        src = ybuf.at[pl.ds(m * rows, rows)]
        return row, pltpu.make_async_copy(src, y_out.at[at.img], lsem), remote(src, y_out.at[at.img], xs.at[m], xr.at[at.img], {'row': row, 'col': at.col})

    def second(m, _):
        acc = conv_rows(at, taps, wbuf.at[1], m * rows)
        y = (xin[pl.ds(m * rows, rows)].astype(F32).reshape(tile, chan) + acc).astype(BF16)
        ybuf[pl.ds(m * rows, rows)] = y.reshape(rows, cols, chan)
        row, local, far = back(m)

        @pl.when(row == at.row)
        def _():
            local.start()

        @pl.when(row != at.row)
        def _():
            far.start()

        return 0

    lax.fori_loop(0, at.seg, second, 0)
    for m in range(at.seg):
        row, local, far = back(m)

        @pl.when(row == at.row)
        def _():
            local.wait()

        @pl.when(row != at.row)
        def _():
            far.wait_send()

    for i in range(at.n_img):
        row = i * at.halves + at.row // at.seg

        @pl.when(row != at.row)
        def _():
            remote(ybuf.at[pl.ds(0, rows)], y_out.at[i], xs.at[0], xr.at[i], {'row': row, 'col': at.col}).wait_recv()


def solution(mesh):
    n_row = mesh.shape['row']
    n_col = mesh.shape['col']

    def run_stage(latent, t_emb, res_norm, res_conv, res_temb, attn_norm, attn_proj):
        n_img, rows, cols, chan = latent.shape
        n_head, dim = attn_proj.shape[1], attn_proj.shape[3]
        dims = (n_img, n_row, n_col, rows, cols, chan)
        halves, seg = n_row // n_img, n_row // (n_row // n_img)
        n_peer = halves * n_col
        own = rows * seg
        tok = own * cols
        per_group = chan // GROUPS
        count = float(n_row * rows * n_col * cols * per_group)
        group_id = np.arange(chan) // per_group
        member = jnp.asarray((group_id[:, None] == group_id[None, :]).astype(np.float32), BF16)
        t_act = jax.nn.silu(t_emb.astype(F32)).astype(BF16)
        temb = jnp.einsum('bk,rkc->rbc', t_act, res_temb, preferred_element_type=F32)
        proj = attn_proj.transpose(0, 1, 3, 2).reshape(4, n_head * dim, chan)

        vmem, anywhere = pl.BlockSpec(memory_space=pltpu.VMEM), pl.BlockSpec(memory_space=pl.ANY)
        block = jax.ShapeDtypeStruct((own, cols, chan), BF16)

        def conv_scratch(n_stage):
            n_msg = n_peer - 1 + 5
            return [
                pltpu.VMEM((own, cols, chan), BF16),
                pltpu.VMEM((own, cols, chan), BF16),
                pltpu.VMEM((own + 2, cols, 3 * chan), BF16),
                pltpu.VMEM((2, 3, 3, chan, chan), BF16),
                pltpu.VMEM((n_stage, 8, chan), F32),
                pltpu.VMEM((n_stage, n_peer, 8, chan), F32),
                pltpu.VMEM((2, cols, chan), BF16),
                pltpu.VMEM((2, 2, own, chan), F32),
                pltpu.VMEM((2, 4, own, chan), F32),
                pltpu.VMEM((4, own, chan), F32),
            ], [
                pltpu.SemaphoreType.DMA((2,)),
                pltpu.SemaphoreType.DMA((n_stage, n_msg)),
                pltpu.SemaphoreType.DMA((n_stage, n_msg)),
                pltpu.SemaphoreType.DMA((max(n_img, seg),)),
                pltpu.SemaphoreType.DMA((max(n_img, seg),)),
                pltpu.SemaphoreType.DMA,
            ]

        def params(cid):
            return pltpu.CompilerParams(collective_id=cid, has_side_effects=True, vmem_limit_bytes=60 << 20)

        bufs, sems = conv_scratch(3)
        x1, every = pl.pallas_call(
            functools.partial(res_first, dims, count, 0),
            out_shape=(block, jax.ShapeDtypeStruct((n_peer, 8, chan), F32)),
            in_specs=[anywhere, vmem, vmem, anywhere, vmem],
            out_specs=(vmem, vmem),
            scratch_shapes=bufs + sems,
            compiler_params=params(0),
            name='res_first',
        )(latent, temb, res_norm, res_conv, member)

        ot = pl.pallas_call(
            functools.partial(attention, dims, count),
            out_shape=jax.ShapeDtypeStruct((chan, tok), BF16),
            in_specs=[vmem] * 5,
            out_specs=vmem,
            scratch_shapes=[
                pltpu.VMEM((n_peer, tok, chan), BF16),
                pltpu.VMEM((n_head, 2 * dim, tok), BF16),
                pltpu.VMEM((2 * tok, chan), BF16),
                pltpu.VMEM((chan, 2 * tok), BF16),
                pltpu.VMEM((2, KEY_BLK, tok), F32),
                pltpu.VMEM((n_head, 8, tok), F32),
                pltpu.VMEM((n_head, 8, tok), F32),
                pltpu.VMEM((n_head, dim, tok), F32),
                pltpu.SemaphoreType.DMA((9,)),
                pltpu.SemaphoreType.DMA((9,)),
                pltpu.SemaphoreType.DMA,
            ],
            compiler_params=params(1),
            name='attention',
        )(x1.reshape(tok, chan), every, attn_norm, proj[:3], member)

        bufs, sems = conv_scratch(2)
        return pl.pallas_call(
            functools.partial(res_second, dims, count, 1),
            out_shape=jax.ShapeDtypeStruct(latent.shape, BF16),
            in_specs=[vmem, vmem, vmem, vmem, vmem, anywhere, vmem],
            out_specs=anywhere,
            scratch_shapes=bufs + [pltpu.VMEM((own, cols, chan), BF16)] + sems,
            compiler_params=params(2),
            name='res_second',
        )(x1, ot, proj[3], temb, res_norm, res_conv, member)

    spec_x = P('dp', 'row', 'col', None)
    return jax.shard_map(run_stage, mesh=mesh, in_specs=(spec_x, P('dp', None), P(), P(), P(), P(), P()), out_specs=spec_x, check_vma=False)
```

```python
import functools

import jax
import jax.numpy as jnp
import numpy as np
from jax import lax
from jax.experimental import pallas as pl
from jax.experimental.pallas import tpu as pltpu
from jax.sharding import PartitionSpec as P

GROUPS = 32
EPS = 1e-5
F32 = jnp.float32
BF16 = jnp.bfloat16
LOG2E = 1.4426950408889634
KEY_BLK = 512
QUERY_TILE = 256


class Place:
    def __init__(self, dims):
        self.n_img, self.n_row, self.n_col, self.rows, self.cols, self.chan = dims
        self.halves = self.n_row // self.n_img
        self.seg = self.n_row // self.halves
        self.row = lax.axis_index('row')
        self.col = lax.axis_index('col')
        self.img = self.row // self.halves
        self.half = self.row % self.halves
        self.n_peer = self.halves * self.n_col
        self.me = self.half * self.n_col + self.col

    def peer(self, step):
        slot = (self.me + step) % self.n_peer
        return {'row': self.img * self.halves + slot // self.n_col, 'col': slot % self.n_col}

    def partner(self):
        return {'row': self.img * self.halves + (1 - self.half), 'col': self.col}

    def beside(self, step, other=False):
        half = (1 - self.half) if other else self.half
        return {'row': self.img * self.halves + half, 'col': (self.col + step + self.n_col) % self.n_col}


def remote(src, dst, send_sem, recv_sem, device):
    return pltpu.make_async_remote_copy(src_ref=src, dst_ref=dst, send_sem=send_sem, recv_sem=recv_sem, device_id=device, device_id_type=pl.DeviceIdType.MESH)


def signal_peers(at, with_column):
    barrier = pltpu.get_barrier_semaphore()
    for step in range(1, at.n_peer):
        pl.semaphore_signal(barrier, inc=1, device_id=at.peer(step), device_id_type=pl.DeviceIdType.MESH)
    count = at.n_peer - 1
    if with_column:
        for step in range(1, at.n_img):
            for half in range(at.halves):
                row = ((at.img + step) % at.n_img) * at.halves + half
                pl.semaphore_signal(barrier, inc=1, device_id={'row': row, 'col': at.col}, device_id_type=pl.DeviceIdType.MESH)
                count += 1
    return count


def wait_peers(count):
    pl.semaphore_wait(pltpu.get_barrier_semaphore(), count)


def stat_copies(at, mine, every, ssem, rsem):
    out = []
    for step in range(1, at.n_peer):
        send = remote(mine, every.at[at.me], ssem.at[step - 1], rsem.at[step - 1], at.peer(step))
        source = (at.me - step + at.n_peer) % at.n_peer
        recv = remote(mine, every.at[source], ssem.at[step - 1], rsem.at[step - 1], at.peer(step))
        out.append((send, recv))
    return out


def halo_copies(at, full, hrow, colbuf, hcol, ssem, rsem):
    base = at.n_peer - 1
    edge = (at.rows * at.seg - 1) * (1 - at.half)
    out = []
    copy = remote(full.at[edge], hrow, ssem.at[base], rsem.at[base], at.partner())
    out.append((copy, copy))
    for slot, (side, step, other) in enumerate([(1, 1, False), (1, 1, True), (0, -1, False), (0, -1, True)]):
        copy = remote(colbuf.at[side], hcol.at[slot], ssem.at[base + 1 + slot], rsem.at[base + 1 + slot], at.beside(step, other))
        out.append((copy, copy))
    return out


def put_stats(stats, mine, every, at):
    s1 = jnp.sum(stats[0], axis=0, keepdims=True)
    s2 = jnp.sum(stats[1], axis=0, keepdims=True)
    idx = lax.broadcasted_iota(jnp.int32, mine.shape, 0)
    both = jnp.where(idx == 0, s1, jnp.where(idx == 1, s2, 0.0))
    mine[...] = both
    every[at.me] = both


def swap_all(at, mine, every, ssem, rsem, full=None, hrow=None, colbuf=None, hcol=None):
    copies = [] if full is None else halo_copies(at, full, hrow, colbuf, hcol, ssem, rsem)
    copies += stat_copies(at, mine, every, ssem, rsem)
    for send, _ in copies:
        send.start()
    for _, recv in copies:
        recv.wait_recv()
    for send, _ in copies:
        send.wait_send()


def norm_terms(every, member, scale, shift, count):
    total = every[0]
    for slot in range(1, every.shape[0]):
        total = total + every[slot]
    high = total.astype(BF16).astype(F32)
    mid = (total - high).astype(BF16).astype(F32)
    low = (total - high - mid).astype(BF16).astype(F32)
    stacked = jnp.concatenate([high, mid, low, jnp.zeros_like(low)], axis=0).astype(BF16)
    n = total.shape[0]
    summed = jnp.dot(stacked, member[...], preferred_element_type=F32)
    sums = summed[0:n] + summed[n:2 * n] + summed[2 * n:3 * n]
    mean = sums[0:1] / count
    var = sums[1:2] / count - mean * mean
    return mean, lax.rsqrt(var + EPS) * scale, shift


def activate(x, terms):
    mean, scale, shift = terms
    u = (x - mean) * scale + shift
    return u / (1.0 + jnp.exp(-u))


def add_stats(stats, vals):
    n, chan = vals.shape
    split = vals.reshape(n // 8, 8, chan)
    return stats[0] + jnp.sum(split, axis=0), stats[1] + jnp.sum(split * split, axis=0)


def zero_stats(chan):
    return jnp.zeros((8, chan), F32), jnp.zeros((8, chan), F32)


def keep_cols(colbuf, first_row, vals, n_rows, cols):
    for k in range(n_rows):
        colbuf[0, pl.ds(first_row + k, 1), :] = vals[k * cols:k * cols + 1]
        colbuf[1, pl.ds(first_row + k, 1), :] = vals[(k + 1) * cols - 1:(k + 1) * cols]


def fill_taps(at, full, hrow, hcol, terms, taps, colact):
    chan, cols = at.chan, at.cols
    n_own = at.rows * at.seg
    for slot in range(4):
        inside = (at.col > 0) if slot < 2 else (at.col < at.n_col - 1)
        colact[slot] = jnp.where(inside, activate(hcol[slot], terms), 0.0)
    row_id = lax.broadcasted_iota(jnp.int32, (cols, chan), 0)

    def put(dst, x, left, right):
        act = activate(x.astype(F32), terms)
        prev = jnp.where(row_id == 0, left, pltpu.roll(act, 1, 0))
        nxt = jnp.where(row_id == cols - 1, right, pltpu.roll(act, cols - 1, 0))
        taps[dst, :, 0:chan] = prev.astype(BF16)
        taps[dst, :, chan:2 * chan] = act.astype(BF16)
        taps[dst, :, 2 * chan:3 * chan] = nxt.astype(BF16)

    def own(r, _):
        put(r + 1, full[r], colact[0, pl.ds(r, 1), :], colact[2, pl.ds(r, 1), :])
        return 0

    lax.fori_loop(0, n_own, own, 0)
    near = (n_own - 1) * at.half
    put((n_own + 1) * (1 - at.half), hrow[...], colact[1, pl.ds(near, 1), :], colact[3, pl.ds(near, 1), :])
    taps[(n_own + 1) * at.half] = jnp.zeros((cols, 3 * chan), BF16)


def conv_rows(at, taps, weights, first):
    acc = None
    for dy in range(3):
        lhs = taps[pl.ds(first + dy, at.rows)].reshape(at.rows * at.cols, 3 * at.chan)
        part = jnp.dot(lhs, weights[dy].reshape(3 * at.chan, at.chan), preferred_element_type=F32)
        acc = part if acc is None else acc + part
    return acc


def norm_rows(ref):
    vals = ref[...].astype(F32)
    return vals[0:1], vals[1:2]


def res_first(dims, count, blk, latent, t_emb, w_temb, norms, w_all, member, x_out, stat_out, xin, hid, taps, wbuf, mine, every, hrow, colbuf, hcol, colact, temb, tbuf, wsem, ssem, rsem, xs, xr, lsem):
    at = Place(dims)
    n_wait = signal_peers(at, True)
    temb_load = pltpu.make_async_copy(w_temb.at[blk], tbuf, wsem.at[2])
    temb_load.start()
    loads = [pltpu.make_async_copy(w_all.at[blk, j], wbuf.at[j], wsem.at[j]) for j in range(2)]
    for load in loads:
        load.start()
    wait_peers(n_wait)
    target_half, slot = at.row // at.seg, at.row % at.seg
    rows, cols, chan = at.rows, at.cols, at.chan
    for i in range(at.n_img):
        row = i * at.halves + target_half
        dst = xin.at[pl.ds(slot * rows, rows)]

        @pl.when(row == at.row)
        def _():
            pltpu.make_async_copy(latent.at[i], dst, lsem).start()

        @pl.when(row != at.row)
        def _():
            remote(latent.at[i], dst, xs.at[i], xr.at[slot], {'row': row, 'col': at.col}).start()

    temb_load.wait()
    time_terms(t_emb, tbuf, temb)
    stats = zero_stats(chan)
    for k in range(at.seg):
        row = at.half * at.seg + k
        dst = xin.at[pl.ds(k * rows, rows)]

        @pl.when(row == at.row)
        def _():
            pltpu.make_async_copy(latent.at[0], dst, lsem).wait()

        @pl.when(row != at.row)
        def _():
            remote(latent.at[0], dst, xs.at[0], xr.at[k], {'row': row, 'col': at.col}).wait_recv()

        vals = xin[k * rows:(k + 1) * rows].astype(F32).reshape(rows * cols, chan)
        stats = add_stats(stats, vals)
        keep_cols(colbuf.at[0], k * rows, vals, rows, cols)
    put_stats(stats, mine.at[0], every.at[0], at)
    swap_all(at, mine.at[0], every.at[0], ssem.at[0], rsem.at[0], xin, hrow.at[0], colbuf.at[0], hcol.at[0])
    for i in range(at.n_img):
        row = i * at.halves + target_half

        @pl.when(row != at.row)
        def _():
            remote(latent.at[i], xin.at[pl.ds(slot * rows, rows)], xs.at[i], xr.at[slot], {'row': row, 'col': at.col}).wait_send()

    conv_pair(at, count, blk, temb, norms, member, xin, hid, taps, wbuf, mine, every, hrow, colbuf, hcol, colact, loads, ssem, rsem)

    def second(m, stats):
        acc = conv_rows(at, taps, wbuf.at[1], m * rows)
        y = (xin[pl.ds(m * rows, rows)].astype(F32).reshape(rows * cols, chan) + acc).astype(BF16)
        x_out[pl.ds(m * rows, rows)] = y.reshape(rows, cols, chan)
        return add_stats(stats, y.astype(F32))

    stats = lax.fori_loop(0, at.seg, second, zero_stats(chan))
    put_stats(stats, mine.at[2], every.at[2], at)
    swap_all(at, mine.at[2], every.at[2], ssem.at[2], rsem.at[2])
    stat_out[...] = every[2]


def conv_pair(at, count, blk, temb, norms, member, xin, hid, taps, wbuf, mine, every, hrow, colbuf, hcol, colact, loads, ssem, rsem):
    rows, cols, chan = at.rows, at.cols, at.chan
    terms = norm_terms(every.at[0], member, *norm_rows(norms.at[blk, 0]), count)
    fill_taps(at, xin, hrow.at[0], hcol.at[0], terms, taps, colact)
    loads[0].wait()
    shift = temb[pl.ds(at.img, 1), :]

    def first(m, stats):
        h = (conv_rows(at, taps, wbuf.at[0], m * rows) + shift).astype(BF16)
        hid[pl.ds(m * rows, rows)] = h.reshape(rows, cols, chan)
        vals = h.astype(F32)
        keep_cols(colbuf.at[1], m * rows, vals, rows, cols)
        return add_stats(stats, vals)

    stats = lax.fori_loop(0, at.seg, first, zero_stats(chan))
    put_stats(stats, mine.at[1], every.at[1], at)
    swap_all(at, mine.at[1], every.at[1], ssem.at[1], rsem.at[1], hid, hrow.at[1], colbuf.at[1], hcol.at[1])
    terms = norm_terms(every.at[1], member, *norm_rows(norms.at[blk, 1]), count)
    fill_taps(at, hid, hrow.at[1], hcol.at[1], terms, taps, colact)
    loads[1].wait()


def time_terms(t_emb, weights, out):
    u = t_emb[...].astype(F32)
    act = (u / (1.0 + jnp.exp(-u))).astype(BF16)
    out[...] = jnp.dot(act, weights[...], preferred_element_type=F32)


def nt(a, b):
    return lax.dot_general(a, b, (((1,), (1,)), ((), ())), preferred_element_type=F32)


def attention(dims, count, x, every, norms, proj_all, member, out, xall, qm, kbuf, vbuf, sbuf, run_max, run_sum, run_out, proj, ssem, rsem, lsem):
    at = Place(dims)
    n_wait = signal_peers(at, False)
    load = pltpu.make_async_copy(proj_all.at[pl.ds(0, 3)], proj, lsem.at[1])
    load.start()
    tok, chan = x.shape
    n_head = qm.shape[0]
    dim = chan // n_head
    half_tok = tok // 2
    own_copy = pltpu.make_async_copy(x, xall.at[0], lsem.at[0])
    own_copy.start()
    terms = norm_terms(every, member, *norm_rows(norms), count)
    right, left, mate = at.beside(1), at.beside(-1), at.partner()
    low, high = pl.ds(0, half_tok), pl.ds(half_tok, half_tok)

    def link(k, src, slot, device):
        return remote(src, slot, ssem.at[k], rsem.at[k], device)

    low_right = link(0, x.at[low], xall.at[1, low], right)
    high_right = link(1, x.at[high], xall.at[2, low], right)
    high_left = link(2, x.at[high], xall.at[1, high], left)
    low_left = link(3, x.at[low], xall.at[2, high], left)
    far_low = link(4, xall.at[1, low], xall.at[3, low], right)
    far_high = link(5, xall.at[1, high], xall.at[3, high], left)
    second = pl.ds(tok, tok)

    def keys_over(k):
        return link(6 + k, kbuf.at[k, pl.ds(0, tok)], kbuf.at[k, second], mate)

    def values_over(k):
        return link(10 + k, vbuf.at[k, :, pl.ds(0, tok)], vbuf.at[k, :, second], mate)

    wait_peers(n_wait)
    low_right.start()
    high_left.start()
    high_right.start()
    low_left.start()
    run_max[...] = jnp.full(run_max.shape, -1e30, F32)
    run_sum[...] = jnp.zeros(run_sum.shape, F32)
    run_out[...] = jnp.zeros(run_out.shape, F32)
    own_copy.wait()
    load.wait()
    first_half = lax.broadcasted_iota(jnp.int32, (tok, 2 * dim), 1) < dim

    def normed(vals):
        return ((vals.astype(F32) - terms[0]) * terms[1] + terms[2]).astype(BF16)

    def project(k, _):
        @pl.when(k == 1)
        def _():
            low_right.wait_recv()
            far_low.start()
            high_left.wait_recv()
            far_high.start()

        @pl.when(k == 2)
        def _():
            high_right.wait_recv()
            low_left.wait_recv()

        @pl.when(k == 3)
        def _():
            far_low.wait_recv()
            far_high.wait_recv()

        g = normed(xall[k])
        keys = nt(g, proj[1])
        for p in range(n_head // 2):
            both = keys[:, p * 2 * dim:(p + 1) * 2 * dim]
            swapped = pltpu.roll(both, dim, 1)
            kbuf[k, 0:tok, 4 * p * dim:(4 * p + 2) * dim] = jnp.where(first_half, both, swapped).astype(BF16)
            kbuf[k, 0:tok, (4 * p + 2) * dim:(4 * p + 4) * dim] = jnp.where(first_half, swapped, both).astype(BF16)
        keys_over(k).start()
        vbuf[k, :, 0:tok] = nt(proj[2], g).astype(BF16)
        values_over(k).start()
        return 0

    def queries():
        qt = nt(proj[0], normed(x[...])).astype(BF16).astype(F32) * (LOG2E * dim ** -0.5)
        hi = qt.astype(BF16)
        rest = qt - hi.astype(F32)
        mid = rest.astype(BF16)
        lo = (rest - mid.astype(F32)).astype(BF16)
        for h in range(n_head):
            rows = slice(h * dim, (h + 1) * dim)
            qm[h, 0:dim, :] = hi[rows]
            qm[h, dim:2 * dim, :] = mid[rows]
            qm[h, 2 * dim:3 * dim, :] = lo[rows]
            qm[h, 3 * dim:4 * dim, :] = jnp.zeros((dim, tok), BF16)

    n_blk = 2 * tok // KEY_BLK

    def attend(k):
        keys_over(k).wait_recv()
        values_over(k).wait_recv()

        def produce(h, j, slot, cols):
            keys = kbuf[k, pl.ds(j * KEY_BLK, KEY_BLK), pl.ds(pl.multiple_of(h * 2 * dim, 2 * dim), 2 * dim)]
            s = jnp.dot(jnp.concatenate([keys, keys], axis=1), qm[h, :, cols], preferred_element_type=F32)
            sbuf[slot, :, cols] = s
            return jnp.max(s.reshape(KEY_BLK // 8, 8, QUERY_TILE), axis=0)

        tiles = [slice(q, q + QUERY_TILE) for q in range(0, tok, QUERY_TILE)]

        def pair(p, tops):
            for u in range(2 * n_blk):
                h, j = 2 * p + u // n_blk, u % n_blk
                if u + 1 < 2 * n_blk:
                    nh, nj = 2 * p + (u + 1) // n_blk, (u + 1) % n_blk
                else:
                    nh, nj = jnp.minimum(2 * p + 2, n_head - 1), 0
                ahead = []
                for q, cols in enumerate(tiles):
                    ahead.append(produce(nh, nj, (u + 1) % 2, cols))
                    m, l, acc = run_max[h, 0:1, cols], run_sum[h, :, cols], run_out[h, :, cols]
                    new = jnp.maximum(m, jnp.max(tops[q], axis=0, keepdims=True))
                    alpha = jnp.exp2(m - new)
                    w = jnp.exp2(sbuf[u % 2, :, cols] - new)
                    run_sum[h, :, cols] = l * alpha + jnp.sum(w.reshape(KEY_BLK // 8, 8, QUERY_TILE), axis=0)
                    run_max[h, 0:1, cols] = new
                    vt = vbuf[k, pl.ds(pl.multiple_of(h * dim, dim), dim), j * KEY_BLK:(j + 1) * KEY_BLK]
                    run_out[h, :, cols] = acc * alpha + jnp.dot(vt, w.astype(BF16), preferred_element_type=F32)
                tops = ahead
            return tuple(tops)

        lax.fori_loop(0, n_head // 2, pair, tuple(produce(0, 0, 0, cols) for cols in tiles))

    def step(i, _):
        @pl.when(i > 0)
        def _():
            attend(i - 1)

        start = jnp.minimum(i + i // 2, 4)
        stop = jnp.minimum((i + 1) + (i + 1) // 2, 4)
        lax.fori_loop(start, stop, project, 0)

        @pl.when(i == 0)
        def _():
            queries()

        return 0

    lax.fori_loop(0, 5, step, 0)
    for copy in (low_right, high_right, high_left, low_left, far_low, far_high):
        copy.wait_send()
    for k in range(4):
        keys_over(k).wait_send()
        values_over(k).wait_send()

    def finish(h, _):
        total = jnp.sum(run_sum[h], axis=0, keepdims=True)
        out[pl.ds(pl.multiple_of(h * dim, dim), dim), :] = (run_out[h] / total).astype(BF16)
        return 0

    lax.fori_loop(0, n_head, finish, 0)


def res_second(dims, count, blk, x, ot, proj_all, t_emb, w_temb, norms, w_all, member, y_out, xin, hid, taps, wbuf, mine, every, hrow, colbuf, hcol, colact, temb, tbuf, ybuf, proj, wsem, ssem, rsem, xs, xr, lsem):
    at = Place(dims)
    n_wait = signal_peers(at, True)
    proj_load = pltpu.make_async_copy(proj_all.at[3], proj, wsem.at[3])
    proj_load.start()
    temb_load = pltpu.make_async_copy(w_temb.at[blk], tbuf, wsem.at[2])
    temb_load.start()
    loads = [pltpu.make_async_copy(w_all.at[blk, j], wbuf.at[j], wsem.at[j]) for j in range(2)]
    for load in loads:
        load.start()
    rows, cols, chan = at.rows, at.cols, at.chan
    tile = rows * cols
    proj_load.wait()
    add = lax.dot_general(ot[...], proj[...], (((0,), (0,)), ((), ())), preferred_element_type=F32)
    stats = zero_stats(chan)
    for m in range(at.seg):
        y = (x[m * rows:(m + 1) * rows].astype(F32).reshape(tile, chan) + add[m * tile:(m + 1) * tile]).astype(BF16)
        xin[m * rows:(m + 1) * rows] = y.reshape(rows, cols, chan)
        vals = y.astype(F32)
        stats = add_stats(stats, vals)
        keep_cols(colbuf.at[0], m * rows, vals, rows, cols)
    put_stats(stats, mine.at[0], every.at[0], at)
    temb_load.wait()
    time_terms(t_emb, tbuf, temb)
    wait_peers(n_wait)
    swap_all(at, mine.at[0], every.at[0], ssem.at[0], rsem.at[0], xin, hrow.at[0], colbuf.at[0], hcol.at[0])
    conv_pair(at, count, blk, temb, norms, member, xin, hid, taps, wbuf, mine, every, hrow, colbuf, hcol, colact, loads, ssem, rsem)

    def back(m):
        row = at.half * at.seg + m
        src = ybuf.at[pl.ds(m * rows, rows)]
        return row, pltpu.make_async_copy(src, y_out.at[at.img], lsem), remote(src, y_out.at[at.img], xs.at[m], xr.at[at.img], {'row': row, 'col': at.col})

    near_first = (1 - ((at.img + 1) // 2) % 2 + at.half) % 2

    def second(t, _):
        m = (t + near_first * (at.seg // 2)) % at.seg
        acc = conv_rows(at, taps, wbuf.at[1], m * rows)
        y = (xin[pl.ds(m * rows, rows)].astype(F32).reshape(tile, chan) + acc).astype(BF16)
        ybuf[pl.ds(m * rows, rows)] = y.reshape(rows, cols, chan)
        row, local, far = back(m)

        @pl.when(row == at.row)
        def _():
            local.start()

        @pl.when(row != at.row)
        def _():
            far.start()

        return 0

    lax.fori_loop(0, at.seg, second, 0)
    for m in range(at.seg):
        row, local, far = back(m)

        @pl.when(row == at.row)
        def _():
            local.wait()

        @pl.when(row != at.row)
        def _():
            far.wait_send()

    for i in range(at.n_img):
        row = i * at.halves + at.row // at.seg

        @pl.when(row != at.row)
        def _():
            remote(ybuf.at[pl.ds(0, rows)], y_out.at[i], xs.at[0], xr.at[i], {'row': row, 'col': at.col}).wait_recv()


def solution(mesh):
    n_row = mesh.shape['row']
    n_col = mesh.shape['col']

    def run_stage(latent, t_emb, res_norm, res_conv, res_temb, attn_norm, attn_proj):
        n_img, rows, cols, chan = latent.shape
        n_head, dim = attn_proj.shape[1], attn_proj.shape[3]
        dims = (n_img, n_row, n_col, rows, cols, chan)
        halves, seg = n_row // n_img, n_row // (n_row // n_img)
        n_peer = halves * n_col
        own = rows * seg
        tok = own * cols
        per_group = chan // GROUPS
        count = float(n_row * rows * n_col * cols * per_group)
        group_id = np.arange(chan) // per_group
        member = jnp.asarray((group_id[:, None] == group_id[None, :]).astype(np.float32), BF16)
        proj = attn_proj.transpose(0, 1, 3, 2).reshape(4, n_head * dim, chan)

        vmem, anywhere = pl.BlockSpec(memory_space=pltpu.VMEM), pl.BlockSpec(memory_space=pl.ANY)
        block = jax.ShapeDtypeStruct((own, cols, chan), BF16)

        def conv_scratch(n_stage):
            n_msg = n_peer - 1 + 5
            return [
                pltpu.VMEM((own, cols, chan), BF16),
                pltpu.VMEM((own, cols, chan), BF16),
                pltpu.VMEM((own + 2, cols, 3 * chan), BF16),
                pltpu.VMEM((2, 3, 3, chan, chan), BF16),
                pltpu.VMEM((n_stage, 8, chan), F32),
                pltpu.VMEM((n_stage, n_peer, 8, chan), F32),
                pltpu.VMEM((2, cols, chan), BF16),
                pltpu.VMEM((2, 2, own, chan), F32),
                pltpu.VMEM((2, 4, own, chan), F32),
                pltpu.VMEM((4, own, chan), F32),
                pltpu.VMEM((n_img, chan), F32),
                pltpu.VMEM(res_temb.shape[1:], BF16),
            ], [
                pltpu.SemaphoreType.DMA((4,)),
                pltpu.SemaphoreType.DMA((n_stage, n_msg)),
                pltpu.SemaphoreType.DMA((n_stage, n_msg)),
                pltpu.SemaphoreType.DMA((max(n_img, seg),)),
                pltpu.SemaphoreType.DMA((max(n_img, seg),)),
                pltpu.SemaphoreType.DMA,
            ]

        def params(cid):
            return pltpu.CompilerParams(collective_id=cid, has_side_effects=True, vmem_limit_bytes=60 << 20)

        bufs, sems = conv_scratch(3)
        x1, every = pl.pallas_call(
            functools.partial(res_first, dims, count, 0),
            out_shape=(block, jax.ShapeDtypeStruct((n_peer, 8, chan), F32)),
            in_specs=[anywhere, vmem, anywhere, vmem, anywhere, vmem],
            out_specs=(vmem, vmem),
            scratch_shapes=bufs + sems,
            compiler_params=params(0),
            name='res_first',
        )(latent, t_emb, res_temb, res_norm, res_conv, member)

        ot = pl.pallas_call(
            functools.partial(attention, dims, count),
            out_shape=jax.ShapeDtypeStruct((chan, tok), BF16),
            in_specs=[vmem, vmem, vmem, anywhere, vmem],
            out_specs=vmem,
            scratch_shapes=[
                pltpu.VMEM((4, tok, chan), BF16),
                pltpu.VMEM((n_head, 4 * dim, tok), BF16),
                pltpu.VMEM((4, 2 * tok, 2 * chan), BF16),
                pltpu.VMEM((4, chan, 2 * tok), BF16),
                pltpu.VMEM((2, KEY_BLK, tok), F32),
                pltpu.VMEM((n_head, 8, tok), F32),
                pltpu.VMEM((n_head, 8, tok), F32),
                pltpu.VMEM((n_head, dim, tok), F32),
                pltpu.VMEM((3, chan, chan), BF16),
                pltpu.SemaphoreType.DMA((14,)),
                pltpu.SemaphoreType.DMA((14,)),
                pltpu.SemaphoreType.DMA((2,)),
            ],
            compiler_params=params(1),
            name='attention',
        )(x1.reshape(tok, chan), every, attn_norm, proj, member)

        bufs, sems = conv_scratch(2)
        return pl.pallas_call(
            functools.partial(res_second, dims, count, 1),
            out_shape=jax.ShapeDtypeStruct(latent.shape, BF16),
            in_specs=[vmem, vmem, anywhere, vmem, anywhere, vmem, anywhere, vmem],
            out_specs=anywhere,
            scratch_shapes=bufs + [pltpu.VMEM((own, cols, chan), BF16), pltpu.VMEM((chan, chan), BF16)] + sems,
            compiler_params=params(2),
            name='res_second',
        )(x1, ot, proj, t_emb, res_temb, res_norm, res_conv, member)

    spec_x = P('dp', 'row', 'col', None)
    return jax.shard_map(run_stage, mesh=mesh, in_specs=(spec_x, P('dp', None), P(), P(), P(), P(), P()), out_specs=spec_x, check_vma=False)
```

```python
import functools

import jax
import jax.numpy as jnp
import numpy as np
from jax import lax
from jax.experimental import pallas as pl
from jax.experimental.pallas import tpu as pltpu
from jax.sharding import PartitionSpec as P

GROUPS = 32
EPS = 1e-5
F32 = jnp.float32
BF16 = jnp.bfloat16
LOG2E = 1.4426950408889634
KEY_BLK = 512
QUERY_TILE = 256


class Place:
    def __init__(self, dims):
        self.n_img, self.n_row, self.n_col, self.rows, self.cols, self.chan = dims
        self.halves = self.n_row // self.n_img
        self.seg = self.n_row // self.halves
        self.row = lax.axis_index('row')
        self.col = lax.axis_index('col')
        self.img = self.row // self.halves
        self.half = self.row % self.halves
        self.n_peer = self.halves * self.n_col
        self.me = self.half * self.n_col + self.col

    def peer(self, step):
        slot = (self.me + step) % self.n_peer
        return {'row': self.img * self.halves + slot // self.n_col, 'col': slot % self.n_col}

    def partner(self):
        return {'row': self.img * self.halves + (1 - self.half), 'col': self.col}

    def beside(self, step, other=False):
        half = (1 - self.half) if other else self.half
        return {'row': self.img * self.halves + half, 'col': (self.col + step + self.n_col) % self.n_col}


def remote(src, dst, send_sem, recv_sem, device):
    return pltpu.make_async_remote_copy(src_ref=src, dst_ref=dst, send_sem=send_sem, recv_sem=recv_sem, device_id=device, device_id_type=pl.DeviceIdType.MESH)


def signal_peers(at, with_column):
    barrier = pltpu.get_barrier_semaphore()
    for step in range(1, at.n_peer):
        pl.semaphore_signal(barrier, inc=1, device_id=at.peer(step), device_id_type=pl.DeviceIdType.MESH)
    count = at.n_peer - 1
    if with_column:
        for step in range(1, at.n_img):
            for half in range(at.halves):
                row = ((at.img + step) % at.n_img) * at.halves + half
                pl.semaphore_signal(barrier, inc=1, device_id={'row': row, 'col': at.col}, device_id_type=pl.DeviceIdType.MESH)
                count += 1
    return count


def wait_peers(count):
    pl.semaphore_wait(pltpu.get_barrier_semaphore(), count)


def stat_copies(at, mine, every, ssem, rsem):
    out = []
    for step in range(1, at.n_peer):
        send = remote(mine, every.at[at.me], ssem.at[step - 1], rsem.at[step - 1], at.peer(step))
        source = (at.me - step + at.n_peer) % at.n_peer
        recv = remote(mine, every.at[source], ssem.at[step - 1], rsem.at[step - 1], at.peer(step))
        out.append((send, recv))
    return out


def halo_copies(at, full, hrow, colbuf, hcol, ssem, rsem):
    base = at.n_peer - 1
    edge = (at.rows * at.seg - 1) * (1 - at.half)
    out = []
    copy = remote(full.at[edge], hrow, ssem.at[base], rsem.at[base], at.partner())
    out.append((copy, copy))
    for slot, (side, step, other) in enumerate([(1, 1, False), (1, 1, True), (0, -1, False), (0, -1, True)]):
        copy = remote(colbuf.at[side], hcol.at[slot], ssem.at[base + 1 + slot], rsem.at[base + 1 + slot], at.beside(step, other))
        out.append((copy, copy))
    return out


def split_dot(vals, matrix):
    high = vals.astype(BF16).astype(F32)
    mid = (vals - high).astype(BF16).astype(F32)
    low = (vals - high - mid).astype(BF16).astype(F32)
    stacked = jnp.concatenate([high, mid, low, jnp.zeros_like(low)], axis=0).astype(BF16)
    out = jnp.dot(stacked, matrix, preferred_element_type=F32)
    return out[0:8] + out[8:16] + out[16:24]


def two_rows(first, second, shape):
    idx = lax.broadcasted_iota(jnp.int32, shape, 0)
    return jnp.where(idx == 0, first, jnp.where(idx == 1, second, 0.0))


def put_stats(stats, mine, every, gather, at):
    s1 = jnp.sum(stats[0], axis=0, keepdims=True)
    s2 = jnp.sum(stats[1], axis=0, keepdims=True)
    groups = split_dot(two_rows(s1, s2, stats[0].shape), gather[...])
    mine[...] = groups
    every[at.me] = groups


def swap_all(at, stats, mine, every, gather, ssem, rsem, full=None, hrow=None, colbuf=None, hcol=None):
    halos = [] if full is None else halo_copies(at, full, hrow, colbuf, hcol, ssem, rsem)
    for send, _ in halos:
        send.start()
    put_stats(stats, mine, every, gather, at)
    sums = stat_copies(at, mine, every, ssem, rsem)
    for send, _ in sums:
        send.start()
    for _, recv in sums + halos:
        recv.wait_recv()
    for send, _ in sums + halos:
        send.wait_send()


def norm_terms(every, spread, scale, shift, count):
    total = every[0]
    for slot in range(1, every.shape[0]):
        total = total + every[slot]
    mean = total[0:1] / count
    inv = lax.rsqrt(total[1:2] / count - mean * mean + EPS)
    wide = split_dot(two_rows(mean, inv, total.shape), spread[...])
    return wide[0:1], wide[1:2] * scale, shift


def activate(x, terms):
    mean, scale, shift = terms
    u = (x - mean) * scale + shift
    return u / (1.0 + jnp.exp(-u))


def add_stats(stats, vals):
    n, chan = vals.shape
    split = vals.reshape(n // 8, 8, chan)
    return stats[0] + jnp.sum(split, axis=0), stats[1] + jnp.sum(split * split, axis=0)


def zero_stats(chan):
    return jnp.zeros((8, chan), F32), jnp.zeros((8, chan), F32)


def keep_cols(colbuf, first_row, vals, n_rows, cols):
    for k in range(n_rows):
        colbuf[0, pl.ds(first_row + k, 1), :] = vals[k * cols:k * cols + 1]
        colbuf[1, pl.ds(first_row + k, 1), :] = vals[(k + 1) * cols - 1:(k + 1) * cols]


def fill_taps(at, full, hrow, hcol, terms, taps, colact):
    chan, cols = at.chan, at.cols
    n_own = at.rows * at.seg
    for slot in range(4):
        inside = (at.col > 0) if slot < 2 else (at.col < at.n_col - 1)
        colact[slot] = jnp.where(inside, activate(hcol[slot], terms), 0.0)
    row_id = lax.broadcasted_iota(jnp.int32, (cols, chan), 0)

    def put(dst, x, left, right):
        act = activate(x.astype(F32), terms)
        prev = jnp.where(row_id == 0, left, pltpu.roll(act, 1, 0))
        nxt = jnp.where(row_id == cols - 1, right, pltpu.roll(act, cols - 1, 0))
        taps[dst, :, 0:chan] = prev.astype(BF16)
        taps[dst, :, chan:2 * chan] = act.astype(BF16)
        taps[dst, :, 2 * chan:3 * chan] = nxt.astype(BF16)

    def own(r, _):
        put(r + 1, full[r], colact[0, pl.ds(r, 1), :], colact[2, pl.ds(r, 1), :])
        return 0

    lax.fori_loop(0, n_own, own, 0)
    near = (n_own - 1) * at.half
    put((n_own + 1) * (1 - at.half), hrow[...], colact[1, pl.ds(near, 1), :], colact[3, pl.ds(near, 1), :])
    taps[(n_own + 1) * at.half] = jnp.zeros((cols, 3 * chan), BF16)


def conv_rows(at, taps, weights, first):
    acc = None
    for dy in range(3):
        lhs = taps[pl.ds(first + dy, at.rows)].reshape(at.rows * at.cols, 3 * at.chan)
        part = jnp.dot(lhs, weights[dy].reshape(3 * at.chan, at.chan), preferred_element_type=F32)
        acc = part if acc is None else acc + part
    return acc


def norm_rows(ref):
    vals = ref[...].astype(F32)
    return vals[0:1], vals[1:2]


def spread_images(at, latent, xin, xs, xr, lsem, colbuf):
    target_half, slot = at.row // at.seg, at.row % at.seg
    rows, cols, chan = at.rows, at.cols, at.chan
    for i in range(at.n_img):
        row = i * at.halves + target_half
        dst = xin.at[pl.ds(slot * rows, rows)]

        @pl.when(row == at.row)
        def _():
            pltpu.make_async_copy(latent.at[i], dst, lsem).start()

        @pl.when(row != at.row)
        def _():
            remote(latent.at[i], dst, xs.at[i], xr.at[slot], {'row': row, 'col': at.col}).start()

    yield
    stats = zero_stats(chan)
    for k in range(at.seg):
        row = at.half * at.seg + k
        dst = xin.at[pl.ds(k * rows, rows)]

        @pl.when(row == at.row)
        def _():
            pltpu.make_async_copy(latent.at[0], dst, lsem).wait()

        @pl.when(row != at.row)
        def _():
            remote(latent.at[0], dst, xs.at[0], xr.at[k], {'row': row, 'col': at.col}).wait_recv()

        vals = xin[k * rows:(k + 1) * rows].astype(F32).reshape(rows * cols, chan)
        stats = add_stats(stats, vals)
        keep_cols(colbuf, k * rows, vals, rows, cols)
    yield stats
    for i in range(at.n_img):
        row = i * at.halves + target_half

        @pl.when(row != at.row)
        def _():
            remote(latent.at[i], xin.at[pl.ds(slot * rows, rows)], xs.at[i], xr.at[slot], {'row': row, 'col': at.col}).wait_send()

    yield


def conv_pair(at, count, blk, stage, halo, temb, norms, gather, spread, xin, hid, taps, wbuf, mine, every, hrow, colbuf, hcol, colact, loads, after_first, ssem, rsem):
    rows, cols, chan = at.rows, at.cols, at.chan
    terms = norm_terms(every.at[stage], spread, *norm_rows(norms.at[blk, 0]), count)
    fill_taps(at, xin, hrow.at[halo], hcol.at[halo], terms, taps, colact)
    loads[0].wait()
    shift = temb[pl.ds(at.img, 1), :]

    def first(m, stats):
        h = (conv_rows(at, taps, wbuf.at[0], m * rows) + shift).astype(BF16)
        hid[pl.ds(m * rows, rows)] = h.reshape(rows, cols, chan)
        vals = h.astype(F32)
        keep_cols(colbuf.at[halo + 1], m * rows, vals, rows, cols)
        return add_stats(stats, vals)

    stats = lax.fori_loop(0, at.seg, first, zero_stats(chan))
    if after_first is not None:
        after_first.start()
    swap_all(at, stats, mine.at[stage + 1], every.at[stage + 1], gather, ssem.at[stage + 1], rsem.at[stage + 1], hid, hrow.at[halo + 1], colbuf.at[halo + 1], hcol.at[halo + 1])
    terms = norm_terms(every.at[stage + 1], spread, *norm_rows(norms.at[blk, 1]), count)
    fill_taps(at, hid, hrow.at[halo + 1], hcol.at[halo + 1], terms, taps, colact)
    loads[1].wait()


def time_terms(t_emb, weights, out):
    u = t_emb[...].astype(F32)
    act = (u / (1.0 + jnp.exp(-u))).astype(BF16)
    out[...] = jnp.dot(act, weights[...], preferred_element_type=F32)


def nt(a, b):
    return lax.dot_general(a, b, (((1,), (1,)), ((), ())), preferred_element_type=F32)


def attention(at, count, every, norms, spread, proj, load, out, xall, kbuf, vbuf, ssem, rsem, qm, sbuf, run_max, run_sum, run_out):
    _, tok, chan = xall.shape
    n_head = qm.shape[0]
    dim = chan // n_head
    half_tok = tok // 2
    x = xall.at[0]
    terms = norm_terms(every, spread, *norm_rows(norms), count)
    right, left, mate = at.beside(1), at.beside(-1), at.partner()
    low, high = pl.ds(0, half_tok), pl.ds(half_tok, half_tok)

    def link(k, src, slot, device):
        return remote(src, slot, ssem.at[k], rsem.at[k], device)

    low_right = link(0, x.at[low], xall.at[1, low], right)
    high_right = link(1, x.at[high], xall.at[2, low], right)
    high_left = link(2, x.at[high], xall.at[1, high], left)
    low_left = link(3, x.at[low], xall.at[2, high], left)
    far_low = link(4, xall.at[1, low], xall.at[3, low], right)
    far_high = link(5, xall.at[1, high], xall.at[3, high], left)
    second = pl.ds(tok, tok)

    def keys_over(k):
        return link(6 + k, kbuf.at[k, pl.ds(0, tok)], kbuf.at[k, second], mate)

    def values_over(k):
        return link(10 + k, vbuf.at[k, :, pl.ds(0, tok)], vbuf.at[k, :, second], mate)

    low_right.start()
    high_left.start()
    high_right.start()
    low_left.start()
    run_max[...] = jnp.full(run_max.shape, -1e30, F32)
    run_sum[...] = jnp.zeros(run_sum.shape, F32)
    run_out[...] = jnp.zeros(run_out.shape, F32)
    load.wait()
    first_half = lax.broadcasted_iota(jnp.int32, (tok, 2 * dim), 1) < dim

    def normed(vals):
        return ((vals.astype(F32) - terms[0]) * terms[1] + terms[2]).astype(BF16)

    def project(k, _):
        @pl.when(k == 1)
        def _():
            low_right.wait_recv()
            far_low.start()
            high_left.wait_recv()
            far_high.start()

        @pl.when(k == 2)
        def _():
            high_right.wait_recv()
            low_left.wait_recv()

        @pl.when(k == 3)
        def _():
            far_low.wait_recv()
            far_high.wait_recv()

        g = normed(xall[k])
        keys = nt(g, proj[1])
        for p in range(n_head // 2):
            both = keys[:, p * 2 * dim:(p + 1) * 2 * dim]
            swapped = pltpu.roll(both, dim, 1)
            kbuf[k, 0:tok, 4 * p * dim:(4 * p + 2) * dim] = jnp.where(first_half, both, swapped).astype(BF16)
            kbuf[k, 0:tok, (4 * p + 2) * dim:(4 * p + 4) * dim] = jnp.where(first_half, swapped, both).astype(BF16)
        keys_over(k).start()
        vbuf[k, :, 0:tok] = nt(proj[2], g).astype(BF16)
        values_over(k).start()
        return 0

    def queries():
        qt = nt(proj[0], normed(x[...])).astype(BF16).astype(F32) * (LOG2E * dim ** -0.5)
        hi = qt.astype(BF16)
        rest = qt - hi.astype(F32)
        mid = rest.astype(BF16)
        lo = (rest - mid.astype(F32)).astype(BF16)
        for h in range(n_head):
            rows = slice(h * dim, (h + 1) * dim)
            qm[h, 0:dim, :] = hi[rows]
            qm[h, dim:2 * dim, :] = mid[rows]
            qm[h, 2 * dim:3 * dim, :] = lo[rows]
            qm[h, 3 * dim:4 * dim, :] = jnp.zeros((dim, tok), BF16)

    n_blk = 2 * tok // KEY_BLK

    def attend(k):
        keys_over(k).wait_recv()
        values_over(k).wait_recv()

        def produce(h, j, slot, cols):
            keys = kbuf[k, pl.ds(j * KEY_BLK, KEY_BLK), pl.ds(pl.multiple_of(h * 2 * dim, 2 * dim), 2 * dim)]
            s = jnp.dot(jnp.concatenate([keys, keys], axis=1), qm[h, :, cols], preferred_element_type=F32)
            sbuf[slot, :, cols] = s
            return jnp.max(s.reshape(KEY_BLK // 8, 8, QUERY_TILE), axis=0)

        tiles = [slice(q, q + QUERY_TILE) for q in range(0, tok, QUERY_TILE)]

        def pair(p, tops):
            for u in range(2 * n_blk):
                h, j = 2 * p + u // n_blk, u % n_blk
                if u + 1 < 2 * n_blk:
                    nh, nj = 2 * p + (u + 1) // n_blk, (u + 1) % n_blk
                else:
                    nh, nj = jnp.minimum(2 * p + 2, n_head - 1), 0
                ahead = []
                for q, cols in enumerate(tiles):
                    ahead.append(produce(nh, nj, (u + 1) % 2, cols))
                    m, l, acc = run_max[h, 0:1, cols], run_sum[h, :, cols], run_out[h, :, cols]
                    new = jnp.maximum(m, jnp.max(tops[q], axis=0, keepdims=True))
                    alpha = jnp.exp2(m - new)
                    w = jnp.exp2(sbuf[u % 2, :, cols] - new)
                    run_sum[h, :, cols] = l * alpha + jnp.sum(w.reshape(KEY_BLK // 8, 8, QUERY_TILE), axis=0)
                    run_max[h, 0:1, cols] = new
                    vt = vbuf[k, pl.ds(pl.multiple_of(h * dim, dim), dim), j * KEY_BLK:(j + 1) * KEY_BLK]
                    run_out[h, :, cols] = acc * alpha + jnp.dot(vt, w.astype(BF16), preferred_element_type=F32)
                tops = ahead
            return tuple(tops)

        lax.fori_loop(0, n_head // 2, pair, tuple(produce(0, 0, 0, cols) for cols in tiles))

    def step(i, _):
        @pl.when(i > 0)
        def _():
            attend(i - 1)

        start = jnp.minimum(i + i // 2, 4)
        stop = jnp.minimum((i + 1) + (i + 1) // 2, 4)
        lax.fori_loop(start, stop, project, 0)

        @pl.when(i == 0)
        def _():
            queries()

        return 0

    lax.fori_loop(0, 5, step, 0)
    for copy in (low_right, high_right, high_left, low_left, far_low, far_high):
        copy.wait_send()
    for k in range(4):
        keys_over(k).wait_send()
        values_over(k).wait_send()

    def finish(h, _):
        total = jnp.sum(run_sum[h], axis=0, keepdims=True)
        out[pl.ds(pl.multiple_of(h * dim, dim), dim), :] = (run_out[h] / total).astype(BF16)
        return 0

    lax.fori_loop(0, n_head, finish, 0)


def stage(dims, count, n_head, latent, t_emb, w_temb, norms, w_all, a_norms, proj_all, gather, spread, y_out, xin, hid, wbuf, mine, every, hrow, colbuf, hcol, colact, temb, tbuf, proj, ot, xall, kbuf, vbuf, wsem, ssem, rsem, xs, xr, ys, yr, lsem, asend, arecv):
    at = Place(dims)
    n_wait = signal_peers(at, True)
    rows, cols, chan = at.rows, at.cols, at.chan
    tile = rows * cols
    tok = tile * at.seg
    loads = [pltpu.make_async_copy(w_all.at[blk, j], wbuf.at[j], wsem.at[2 * blk + j]) for blk in range(2) for j in range(2)]
    temb_loads = [pltpu.make_async_copy(w_temb.at[blk], tbuf, wsem.at[4 + blk]) for blk in range(2)]
    proj_load = pltpu.make_async_copy(proj_all, proj, wsem.at[6])
    wait_peers(n_wait)
    images = spread_images(at, latent, xin, xs, xr, lsem, colbuf.at[0])
    next(images)
    temb_loads[0].start()
    loads[0].start()
    loads[1].start()
    proj_load.start()
    temb_loads[0].wait()
    time_terms(t_emb, tbuf, temb)
    temb_loads[1].start()
    stats = next(images)
    swap_all(at, stats, mine.at[0], every.at[0], gather, ssem.at[0], rsem.at[0], xin, hrow.at[0], colbuf.at[0], hcol.at[0])
    next(images)
    tap_shape = pltpu.VMEM((rows * at.seg + 2, cols, 3 * chan), BF16)

    def first_block(taps):
        conv_pair(at, count, 0, 0, 0, temb, norms, gather, spread, xin, hid, taps, wbuf, mine, every, hrow, colbuf, hcol, colact, loads[0:2], loads[2], ssem, rsem)

        def second(m, stats):
            acc = conv_rows(at, taps, wbuf.at[1], m * rows)
            y = (xin[pl.ds(m * rows, rows)].astype(F32).reshape(tile, chan) + acc).astype(BF16)
            xall[0, pl.ds(m * tile, tile)] = y
            return add_stats(stats, y.astype(F32))

        stats = lax.fori_loop(0, at.seg, second, zero_stats(chan))
        loads[3].start()
        swap_all(at, stats, mine.at[2], every.at[2], gather, ssem.at[2], rsem.at[2])

    pl.run_scoped(first_block, tap_shape)
    dim = chan // n_head
    pl.run_scoped(
        functools.partial(attention, at, count, every.at[2], a_norms, spread, proj, proj_load, ot, xall, kbuf, vbuf, asend, arecv),
        pltpu.VMEM((n_head, 4 * dim, tok), BF16),
        pltpu.VMEM((2, KEY_BLK, tok), F32),
        pltpu.VMEM((n_head, 8, tok), F32),
        pltpu.VMEM((n_head, 8, tok), F32),
        pltpu.VMEM((n_head, dim, tok), F32),
    )
    temb_loads[1].wait()
    time_terms(t_emb, tbuf, temb)
    pl.run_scoped(functools.partial(second_block, at, count, norms, gather, spread, y_out, xin, hid, wbuf, mine, every, hrow, colbuf, hcol, colact, temb, proj, ot, xall, loads, ssem, rsem, ys, yr, lsem), tap_shape)


def second_block(at, count, norms, gather, spread, y_out, xin, hid, wbuf, mine, every, hrow, colbuf, hcol, colact, temb, proj, ot, xall, loads, ssem, rsem, xs, xr, lsem, taps):
    rows, cols, chan = at.rows, at.cols, at.chan
    tile = rows * cols
    add = lax.dot_general(ot[...], proj[3], (((0,), (0,)), ((), ())), preferred_element_type=F32)
    stats = zero_stats(chan)
    for m in range(at.seg):
        y = (xall[0, m * tile:(m + 1) * tile].astype(F32) + add[m * tile:(m + 1) * tile]).astype(BF16)
        xin[m * rows:(m + 1) * rows] = y.reshape(rows, cols, chan)
        vals = y.astype(F32)
        stats = add_stats(stats, vals)
        keep_cols(colbuf.at[2], m * rows, vals, rows, cols)
    swap_all(at, stats, mine.at[3], every.at[3], gather, ssem.at[3], rsem.at[3], xin, hrow.at[2], colbuf.at[2], hcol.at[2])
    conv_pair(at, count, 1, 3, 2, temb, norms, gather, spread, xin, hid, taps, wbuf, mine, every, hrow, colbuf, hcol, colact, loads[2:4], None, ssem, rsem)
    ybuf = hid

    def back(m):
        row = at.half * at.seg + m
        src = ybuf.at[pl.ds(m * rows, rows)]
        return row, pltpu.make_async_copy(src, y_out.at[at.img], lsem), remote(src, y_out.at[at.img], xs.at[m], xr.at[at.img], {'row': row, 'col': at.col})

    near_first = (1 - ((at.img + 1) // 2) % 2 + at.half) % 2

    def second(t, _):
        m = (t + near_first * (at.seg // 2)) % at.seg
        acc = conv_rows(at, taps, wbuf.at[1], m * rows)
        y = (xin[pl.ds(m * rows, rows)].astype(F32).reshape(tile, chan) + acc).astype(BF16)
        ybuf[pl.ds(m * rows, rows)] = y.reshape(rows, cols, chan)
        row, local, far = back(m)

        @pl.when(row == at.row)
        def _():
            local.start()

        @pl.when(row != at.row)
        def _():
            far.start()

        return 0

    lax.fori_loop(0, at.seg, second, 0)
    for m in range(at.seg):
        row, local, far = back(m)

        @pl.when(row == at.row)
        def _():
            local.wait()

        @pl.when(row != at.row)
        def _():
            far.wait_send()

    for i in range(at.n_img):
        row = i * at.halves + at.row // at.seg

        @pl.when(row != at.row)
        def _():
            remote(ybuf.at[pl.ds(0, rows)], y_out.at[i], xs.at[0], xr.at[i], {'row': row, 'col': at.col}).wait_recv()


def solution(mesh):
    n_row = mesh.shape['row']
    n_col = mesh.shape['col']

    def run_stage(latent, t_emb, res_norm, res_conv, res_temb, attn_norm, attn_proj):
        n_img, rows, cols, chan = latent.shape
        n_head, dim = attn_proj.shape[1], attn_proj.shape[3]
        dims = (n_img, n_row, n_col, rows, cols, chan)
        halves, seg = n_row // n_img, n_row // (n_row // n_img)
        n_peer = halves * n_col
        own = rows * seg
        tok = own * cols
        per_group = chan // GROUPS
        count = float(n_row * rows * n_col * cols * per_group)
        group_id = np.arange(chan) // per_group
        member = (group_id[:, None] == np.arange(128)[None, :]).astype(np.float32)
        proj = attn_proj.transpose(0, 1, 3, 2).reshape(4, n_head * dim, chan)
        n_msg = n_peer - 1 + 5
        n_stage = 5
        vmem, anywhere = pl.BlockSpec(memory_space=pltpu.VMEM), pl.BlockSpec(memory_space=pl.ANY)
        return pl.pallas_call(
            functools.partial(stage, dims, count, n_head),
            out_shape=jax.ShapeDtypeStruct(latent.shape, BF16),
            in_specs=[anywhere, vmem, anywhere, vmem, anywhere, vmem, anywhere, vmem, vmem],
            out_specs=anywhere,
            scratch_shapes=[
                pltpu.VMEM((own, cols, chan), BF16),
                pltpu.VMEM((own, cols, chan), BF16),
                pltpu.VMEM((2, 3, 3, chan, chan), BF16),
                pltpu.VMEM((n_stage, 8, 128), F32),
                pltpu.VMEM((n_stage, n_peer, 8, 128), F32),
                pltpu.VMEM((4, cols, chan), BF16),
                pltpu.VMEM((4, 2, own, chan), F32),
                pltpu.VMEM((4, 4, own, chan), F32),
                pltpu.VMEM((4, own, chan), F32),
                pltpu.VMEM((n_img, chan), F32),
                pltpu.VMEM(res_temb.shape[1:], BF16),
                pltpu.VMEM((4, n_head * dim, chan), BF16),
                pltpu.VMEM((n_head * dim, tok), BF16),
                pltpu.VMEM((4, tok, chan), BF16),
                pltpu.VMEM((4, 2 * tok, 2 * chan), BF16),
                pltpu.VMEM((4, chan, 2 * tok), BF16),
                pltpu.SemaphoreType.DMA((7,)),
                pltpu.SemaphoreType.DMA((n_stage, n_msg)),
                pltpu.SemaphoreType.DMA((n_stage, n_msg)),
                pltpu.SemaphoreType.DMA((n_img,)),
                pltpu.SemaphoreType.DMA((seg,)),
                pltpu.SemaphoreType.DMA((seg,)),
                pltpu.SemaphoreType.DMA((n_img,)),
                pltpu.SemaphoreType.DMA,
                pltpu.SemaphoreType.DMA((14,)),
                pltpu.SemaphoreType.DMA((14,)),
            ],
            compiler_params=pltpu.CompilerParams(collective_id=0, has_side_effects=True, vmem_limit_bytes=67043328),
            name='unet_stage',
        )(latent, t_emb, res_temb, res_norm, res_conv, attn_norm, proj, jnp.asarray(member, BF16), jnp.asarray(member.T.copy(), BF16))

    spec_x = P('dp', 'row', 'col', None)
    return jax.shard_map(run_stage, mesh=mesh, in_specs=(spec_x, P('dp', None), P(), P(), P(), P(), P()), out_specs=spec_x, check_vma=False)
```

```python
import functools

import jax
import jax.numpy as jnp
import numpy as np
from jax import lax
from jax.experimental import pallas as pl
from jax.experimental.pallas import tpu as pltpu
from jax.sharding import PartitionSpec as P

GROUPS = 32
EPS = 1e-5
F32 = jnp.float32
BF16 = jnp.bfloat16
LOG2E = 1.4426950408889634
KEY_BLK = 512
QUERY_TILE = 256
HEADS_PER_STEP = 5


class Place:
    def __init__(self, dims):
        self.n_img, self.n_row, self.n_col, self.rows, self.cols, self.chan = dims
        self.halves = self.n_row // self.n_img
        self.seg = self.n_row // self.halves
        self.row = lax.axis_index('row')
        self.col = lax.axis_index('col')
        self.img = self.row // self.halves
        self.half = self.row % self.halves
        self.n_peer = self.halves * self.n_col
        self.me = self.half * self.n_col + self.col

    def peer(self, step):
        slot = (self.me + step) % self.n_peer
        return {'row': self.img * self.halves + slot // self.n_col, 'col': slot % self.n_col}

    def partner(self):
        return {'row': self.img * self.halves + (1 - self.half), 'col': self.col}

    def beside(self, step, other=False):
        half = (1 - self.half) if other else self.half
        return {'row': self.img * self.halves + half, 'col': (self.col + step + self.n_col) % self.n_col}


def remote(src, dst, send_sem, recv_sem, device):
    return pltpu.make_async_remote_copy(src_ref=src, dst_ref=dst, send_sem=send_sem, recv_sem=recv_sem, device_id=device, device_id_type=pl.DeviceIdType.MESH)


def signal_peers(at, with_column):
    barrier = pltpu.get_barrier_semaphore()
    for step in range(1, at.n_peer):
        pl.semaphore_signal(barrier, inc=1, device_id=at.peer(step), device_id_type=pl.DeviceIdType.MESH)
    count = at.n_peer - 1
    if with_column:
        for step in range(1, at.n_img):
            for half in range(at.halves):
                row = ((at.img + step) % at.n_img) * at.halves + half
                pl.semaphore_signal(barrier, inc=1, device_id={'row': row, 'col': at.col}, device_id_type=pl.DeviceIdType.MESH)
                count += 1
    return count


def wait_peers(count):
    pl.semaphore_wait(pltpu.get_barrier_semaphore(), count)


def stat_copies(at, mine, every, ssem, rsem):
    out = []
    for step in range(1, at.n_peer):
        send = remote(mine, every.at[at.me], ssem.at[step - 1], rsem.at[step - 1], at.peer(step))
        source = (at.me - step + at.n_peer) % at.n_peer
        recv = remote(mine, every.at[source], ssem.at[step - 1], rsem.at[step - 1], at.peer(step))
        out.append((send, recv))
    return out


def halo_copies(at, full, hrow, colbuf, hcol, ssem, rsem):
    base = at.n_peer - 1
    edge = (at.rows * at.seg - 1) * (1 - at.half)
    out = []
    copy = remote(full.at[edge], hrow, ssem.at[base], rsem.at[base], at.partner())
    out.append((copy, copy))
    for slot, (side, step, other) in enumerate([(1, 1, False), (1, 1, True), (0, -1, False), (0, -1, True)]):
        copy = remote(colbuf.at[side], hcol.at[slot], ssem.at[base + 1 + slot], rsem.at[base + 1 + slot], at.beside(step, other))
        out.append((copy, copy))
    return out


def split_dot(vals, matrix):
    high = vals.astype(BF16).astype(F32)
    mid = (vals - high).astype(BF16).astype(F32)
    low = (vals - high - mid).astype(BF16).astype(F32)
    stacked = jnp.concatenate([high, mid, low, jnp.zeros_like(low)], axis=0).astype(BF16)
    out = jnp.dot(stacked, matrix, preferred_element_type=F32)
    return out[0:8] + out[8:16] + out[16:24]


def two_rows(first, second, shape):
    idx = lax.broadcasted_iota(jnp.int32, shape, 0)
    return jnp.where(idx == 0, first, jnp.where(idx == 1, second, 0.0))


def put_stats(stats, mine, every, gather, at):
    s1 = jnp.sum(stats[0], axis=0, keepdims=True)
    s2 = jnp.sum(stats[1], axis=0, keepdims=True)
    groups = split_dot(two_rows(s1, s2, stats[0].shape), gather[...])
    mine[...] = groups
    every[at.me] = groups


def swap_all(at, stats, mine, every, gather, ssem, rsem, full=None, hrow=None, colbuf=None, hcol=None, behind=()):
    halos = [] if full is None else halo_copies(at, full, hrow, colbuf, hcol, ssem, rsem)
    for send, _ in halos:
        send.start()
    put_stats(stats, mine, every, gather, at)
    sums = stat_copies(at, mine, every, ssem, rsem)
    for send, _ in sums:
        send.start()
    for copy in behind:
        copy.start()
    for _, recv in sums + halos:
        recv.wait_recv()
    for send, _ in sums + halos:
        send.wait_send()


def norm_terms(every, spread, scale, shift, count):
    total = every[0]
    for slot in range(1, every.shape[0]):
        total = total + every[slot]
    mean = total[0:1] / count
    inv = lax.rsqrt(total[1:2] / count - mean * mean + EPS)
    wide = split_dot(two_rows(mean, inv, total.shape), spread[...])
    return wide[0:1], wide[1:2] * scale, shift


def activate(x, terms):
    mean, scale, shift = terms
    half = ((x - mean) * scale + shift) * 0.5
    return half + half * jnp.tanh(half)


def add_stats(stats, vals):
    n, chan = vals.shape
    split = vals.reshape(n // 8, 8, chan)
    return stats[0] + jnp.sum(split, axis=0), stats[1] + jnp.sum(split * split, axis=0)


def zero_stats(chan):
    return jnp.zeros((8, chan), F32), jnp.zeros((8, chan), F32)


def keep_cols(colbuf, first_row, vals, n_rows, cols):
    for k in range(n_rows):
        colbuf[0, pl.ds(first_row + k, 1), :] = vals[k * cols:k * cols + 1]
        colbuf[1, pl.ds(first_row + k, 1), :] = vals[(k + 1) * cols - 1:(k + 1) * cols]


def fill_taps(at, full, hrow, hcol, terms, taps, colact):
    chan, cols = at.chan, at.cols
    n_own = at.rows * at.seg
    for slot in range(4):
        inside = (at.col > 0) if slot < 2 else (at.col < at.n_col - 1)
        colact[slot] = jnp.where(inside, activate(hcol[slot], terms), 0.0)
    row_id = lax.broadcasted_iota(jnp.int32, (cols, chan), 0)

    def put(dst, x, left, right):
        act = activate(x.astype(F32), terms)
        prev = jnp.where(row_id == 0, left, pltpu.roll(act, 1, 0))
        nxt = jnp.where(row_id == cols - 1, right, pltpu.roll(act, cols - 1, 0))
        taps[dst, :, 0:chan] = prev.astype(BF16)
        taps[dst, :, chan:2 * chan] = act.astype(BF16)
        taps[dst, :, 2 * chan:3 * chan] = nxt.astype(BF16)

    def own(r, _):
        put(r + 1, full[r], colact[0, pl.ds(r, 1), :], colact[2, pl.ds(r, 1), :])
        return 0

    lax.fori_loop(0, n_own, own, 0)
    near = (n_own - 1) * at.half
    put((n_own + 1) * (1 - at.half), hrow[...], colact[1, pl.ds(near, 1), :], colact[3, pl.ds(near, 1), :])
    taps[(n_own + 1) * at.half] = jnp.zeros((cols, 3 * chan), BF16)


def conv_rows(at, taps, weights, first):
    acc = None
    for dy in range(3):
        lhs = taps[pl.ds(first + dy, at.rows)].reshape(at.rows * at.cols, 3 * at.chan)
        part = jnp.dot(lhs, weights[dy].reshape(3 * at.chan, at.chan), preferred_element_type=F32)
        acc = part if acc is None else acc + part
    return acc


def norm_rows(ref):
    vals = ref[...].astype(F32)
    return vals[0:1], vals[1:2]


def spread_images(at, latent, xin, xs, xr, lsem, colbuf):
    target_half, slot = at.row // at.seg, at.row % at.seg
    rows, cols, chan = at.rows, at.cols, at.chan
    for i in range(at.n_img):
        row = i * at.halves + target_half
        dst = xin.at[pl.ds(slot * rows, rows)]

        @pl.when(row == at.row)
        def _():
            pltpu.make_async_copy(latent.at[i], dst, lsem).start()

        @pl.when(row != at.row)
        def _():
            remote(latent.at[i], dst, xs.at[i], xr.at[slot], {'row': row, 'col': at.col}).start()

    yield
    stats = zero_stats(chan)
    for k in range(at.seg):
        row = at.half * at.seg + k
        dst = xin.at[pl.ds(k * rows, rows)]

        @pl.when(row == at.row)
        def _():
            pltpu.make_async_copy(latent.at[0], dst, lsem).wait()

        @pl.when(row != at.row)
        def _():
            remote(latent.at[0], dst, xs.at[0], xr.at[k], {'row': row, 'col': at.col}).wait_recv()

        vals = xin[k * rows:(k + 1) * rows].astype(F32).reshape(rows * cols, chan)
        stats = add_stats(stats, vals)
        keep_cols(colbuf, k * rows, vals, rows, cols)
    yield stats
    for i in range(at.n_img):
        row = i * at.halves + target_half

        @pl.when(row != at.row)
        def _():
            remote(latent.at[i], xin.at[pl.ds(slot * rows, rows)], xs.at[i], xr.at[slot], {'row': row, 'col': at.col}).wait_send()

    yield


def conv_pair(at, count, blk, stage, halo, temb, norms, gather, spread, xin, hid, taps, wbuf, mine, every, hrow, colbuf, hcol, colact, loads, after_first, ssem, rsem):
    rows, cols, chan = at.rows, at.cols, at.chan
    terms = norm_terms(every.at[stage], spread, *norm_rows(norms.at[blk, 0]), count)
    fill_taps(at, xin, hrow.at[halo], hcol.at[halo], terms, taps, colact)
    loads[0].wait()
    shift = temb[pl.ds(at.img, 1), :]

    def first(m, stats):
        h = (conv_rows(at, taps, wbuf.at[0], m * rows) + shift).astype(BF16)
        hid[pl.ds(m * rows, rows)] = h.reshape(rows, cols, chan)
        vals = h.astype(F32)
        keep_cols(colbuf.at[halo + 1], m * rows, vals, rows, cols)
        return add_stats(stats, vals)

    stats = lax.fori_loop(0, at.seg, first, zero_stats(chan))
    if after_first is not None:
        after_first.start()
    swap_all(at, stats, mine.at[stage + 1], every.at[stage + 1], gather, ssem.at[stage + 1], rsem.at[stage + 1], hid, hrow.at[halo + 1], colbuf.at[halo + 1], hcol.at[halo + 1])
    terms = norm_terms(every.at[stage + 1], spread, *norm_rows(norms.at[blk, 1]), count)
    fill_taps(at, hid, hrow.at[halo + 1], hcol.at[halo + 1], terms, taps, colact)
    loads[1].wait()


def time_terms(t_emb, weights, out):
    u = t_emb[...].astype(F32)
    act = (u / (1.0 + jnp.exp(-u))).astype(BF16)
    out[...] = jnp.dot(act, weights[...], preferred_element_type=F32)


def nt(a, b):
    return lax.dot_general(a, b, (((1,), (1,)), ((), ())), preferred_element_type=F32)


def gather_links(at, xall, ssem, rsem):
    half_tok = xall.shape[1] // 2
    right, left = at.beside(1), at.beside(-1)
    low, high = pl.ds(0, half_tok), pl.ds(half_tok, half_tok)
    x = xall.at[0]
    ends = [(x.at[low], xall.at[1, low], right), (x.at[high], xall.at[2, low], right), (x.at[high], xall.at[1, high], left), (x.at[low], xall.at[2, high], left), (xall.at[1, low], xall.at[3, low], right), (xall.at[1, high], xall.at[3, high], left)]
    return [remote(src, dst, ssem.at[k], rsem.at[k], device) for k, (src, dst, device) in enumerate(ends)]


def attention(at, count, every, norms, spread, proj, load, meanwhile, out, xall, kbuf, vbuf, ssem, rsem, qm, sbuf, run_max, run_sum, run_out):
    _, tok, chan = xall.shape
    n_head = qm.shape[0]
    dim = chan // n_head
    x = xall.at[0]
    terms = norm_terms(every, spread, *norm_rows(norms), count)
    mate = at.partner()

    def link(k, src, slot, device):
        return remote(src, slot, ssem.at[k], rsem.at[k], device)

    low_right, high_right, high_left, low_left, far_low, far_high = gather_links(at, xall, ssem, rsem)
    second = pl.ds(tok, tok)

    def keys_over(k):
        return link(6 + k, kbuf.at[k, pl.ds(0, tok)], kbuf.at[k, second], mate)

    def values_over(k):
        return link(10 + k, vbuf.at[k, :, pl.ds(0, tok)], vbuf.at[k, :, second], mate)

    load.wait()
    first_half = lax.broadcasted_iota(jnp.int32, (tok, 2 * dim), 1) < dim

    def normed(vals):
        return ((vals.astype(F32) - terms[0]) * terms[1] + terms[2]).astype(BF16)

    def project(k, _):
        @pl.when(k == 1)
        def _():
            low_right.wait_recv()
            far_low.start()
            high_left.wait_recv()
            far_high.start()

        @pl.when(k == 2)
        def _():
            high_right.wait_recv()
            low_left.wait_recv()

        @pl.when(k == 3)
        def _():
            far_low.wait_recv()
            far_high.wait_recv()

        g = normed(xall[k])
        keys = nt(g, proj[1])
        for p in range(n_head // 2):
            both = keys[:, p * 2 * dim:(p + 1) * 2 * dim]
            swapped = pltpu.roll(both, dim, 1)
            kbuf[k, 0:tok, 4 * p * dim:(4 * p + 2) * dim] = jnp.where(first_half, both, swapped).astype(BF16)
            kbuf[k, 0:tok, (4 * p + 2) * dim:(4 * p + 4) * dim] = jnp.where(first_half, swapped, both).astype(BF16)
        keys_over(k).start()
        vbuf[k, :, 0:tok] = nt(proj[2], g).astype(BF16)
        values_over(k).start()
        return 0

    def queries():
        run_max[...] = jnp.full(run_max.shape, -1e30, F32)
        run_sum[...] = jnp.zeros(run_sum.shape, F32)
        run_out[...] = jnp.zeros(run_out.shape, F32)
        meanwhile()
        qt = nt(proj[0], normed(x[...])).astype(BF16).astype(F32) * (LOG2E * dim ** -0.5)
        hi = qt.astype(BF16)
        rest = qt - hi.astype(F32)
        mid = rest.astype(BF16)
        lo = (rest - mid.astype(F32)).astype(BF16)
        for h in range(n_head):
            rows = slice(h * dim, (h + 1) * dim)
            qm[h, 0:dim, :] = hi[rows]
            qm[h, dim:2 * dim, :] = mid[rows]
            qm[h, 2 * dim:3 * dim, :] = lo[rows]
            qm[h, 3 * dim:4 * dim, :] = jnp.zeros((dim, tok), BF16)

    n_blk = 2 * tok // KEY_BLK
    n_slot = sbuf.shape[0]
    assert HEADS_PER_STEP * n_blk % n_slot == 0

    def attend(k):
        keys_over(k).wait_recv()
        values_over(k).wait_recv()

        def produce(h, j, slot, cols):
            keys = kbuf[k, pl.ds(j * KEY_BLK, KEY_BLK), pl.ds(pl.multiple_of(h * 2 * dim, 2 * dim), 2 * dim)]
            s = jnp.dot(jnp.concatenate([keys, keys], axis=1), qm[h, :, cols], preferred_element_type=F32)
            sbuf[slot, :, cols] = s
            return jnp.max(s.reshape(KEY_BLK // 8, 8, QUERY_TILE), axis=0)

        tiles = [slice(q, q + QUERY_TILE) for q in range(0, tok, QUERY_TILE)]

        def heads(p, tops):
            for u in range(HEADS_PER_STEP * n_blk):
                h, j = HEADS_PER_STEP * p + u // n_blk, u % n_blk
                nh, nj = HEADS_PER_STEP * p + (u + 1) // n_blk, (u + 1) % n_blk
                if u + 1 == HEADS_PER_STEP * n_blk:
                    nh = jnp.minimum(nh, n_head - 1)
                ahead = []
                for q, cols in enumerate(tiles):
                    ahead.append(produce(nh, nj, (u + 1) % n_slot, cols))
                    m, l, acc = run_max[h, 0:1, cols], run_sum[h, :, cols], run_out[h, :, cols]
                    new = jnp.maximum(m, jnp.max(tops[q], axis=0, keepdims=True))
                    alpha = jnp.exp2(m - new)
                    w = jnp.exp2(sbuf[u % n_slot, :, cols] - new)
                    run_sum[h, :, cols] = l * alpha + jnp.sum(w.reshape(KEY_BLK // 8, 8, QUERY_TILE), axis=0)
                    run_max[h, 0:1, cols] = new
                    vt = vbuf[k, pl.ds(pl.multiple_of(h * dim, dim), dim), j * KEY_BLK:(j + 1) * KEY_BLK]
                    run_out[h, :, cols] = acc * alpha + jnp.dot(vt, w.astype(BF16), preferred_element_type=F32)
                tops = ahead
            return tuple(tops)

        lax.fori_loop(0, n_head // HEADS_PER_STEP, heads, tuple(produce(0, 0, 0, cols) for cols in tiles))

    def step(i, _):
        @pl.when(i > 0)
        def _():
            attend(i - 1)

        start = jnp.minimum(i + i // 2, 4)
        stop = jnp.minimum((i + 1) + (i + 1) // 2, 4)
        lax.fori_loop(start, stop, project, 0)

        @pl.when(i == 0)
        def _():
            queries()

        return 0

    lax.fori_loop(0, 5, step, 0)
    for copy in (low_right, high_right, high_left, low_left, far_low, far_high):
        copy.wait_send()
    for k in range(4):
        keys_over(k).wait_send()
        values_over(k).wait_send()

    def finish(h, _):
        total = jnp.sum(run_sum[h], axis=0, keepdims=True)
        out[pl.ds(pl.multiple_of(h * dim, dim), dim), :] = (run_out[h] / total).astype(BF16)
        return 0

    lax.fori_loop(0, n_head, finish, 0)


def stage(dims, count, n_head, latent, t_emb, w_temb, norms, w_all, a_norms, proj_all, gather, spread, y_out, xin, hid, wbuf, mine, every, hrow, colbuf, hcol, colact, temb, tbuf, proj, ot, xall, kbuf, vbuf, wsem, ssem, rsem, xs, xr, ys, yr, lsem, asend, arecv):
    at = Place(dims)
    n_wait = signal_peers(at, True)
    rows, cols, chan = at.rows, at.cols, at.chan
    tile = rows * cols
    tok = tile * at.seg
    loads = [pltpu.make_async_copy(w_all.at[blk, j], wbuf.at[j], wsem.at[2 * blk + j]) for blk in range(2) for j in range(2)]
    temb_loads = [pltpu.make_async_copy(w_temb.at[blk], tbuf, wsem.at[4 + blk]) for blk in range(2)]
    proj_load = pltpu.make_async_copy(proj_all, proj, wsem.at[6])
    wait_peers(n_wait)
    images = spread_images(at, latent, xin, xs, xr, lsem, colbuf.at[0])
    next(images)
    temb_loads[0].start()
    loads[0].start()
    loads[1].start()
    proj_load.start()
    temb_loads[0].wait()
    time_terms(t_emb, tbuf, temb)
    temb_loads[1].start()
    stats = next(images)
    swap_all(at, stats, mine.at[0], every.at[0], gather, ssem.at[0], rsem.at[0], xin, hrow.at[0], colbuf.at[0], hcol.at[0])
    next(images)
    tap_shape = pltpu.VMEM((rows * at.seg + 2, cols, 3 * chan), BF16)

    def first_block(taps):
        conv_pair(at, count, 0, 0, 0, temb, norms, gather, spread, xin, hid, taps, wbuf, mine, every, hrow, colbuf, hcol, colact, loads[0:2], loads[2], ssem, rsem)

        def second(m, stats):
            acc = conv_rows(at, taps, wbuf.at[1], m * rows)
            y = (xin[pl.ds(m * rows, rows)].astype(F32).reshape(tile, chan) + acc).astype(BF16)
            xall[0, pl.ds(m * tile, tile)] = y
            return add_stats(stats, y.astype(F32))

        stats = lax.fori_loop(0, at.seg, second, zero_stats(chan))
        loads[3].start()
        links = gather_links(at, xall, asend, arecv)
        swap_all(at, stats, mine.at[2], every.at[2], gather, ssem.at[2], rsem.at[2], behind=(links[0], links[2], links[1], links[3]))

    pl.run_scoped(first_block, tap_shape)

    def next_time():
        temb_loads[1].wait()
        time_terms(t_emb, tbuf, temb)

    dim = chan // n_head
    pl.run_scoped(
        functools.partial(attention, at, count, every.at[2], a_norms, spread, proj, proj_load, next_time, ot, xall, kbuf, vbuf, asend, arecv),
        pltpu.VMEM((n_head, 4 * dim, tok), BF16),
        pltpu.VMEM((3, KEY_BLK, tok), F32),
        pltpu.VMEM((n_head, 8, tok), F32),
        pltpu.VMEM((n_head, 8, tok), F32),
        pltpu.VMEM((n_head, dim, tok), F32),
    )
    pl.run_scoped(functools.partial(second_block, at, count, norms, gather, spread, y_out, xin, hid, wbuf, mine, every, hrow, colbuf, hcol, colact, temb, proj, ot, xall, loads, ssem, rsem, ys, yr, lsem), tap_shape)


def second_block(at, count, norms, gather, spread, y_out, xin, hid, wbuf, mine, every, hrow, colbuf, hcol, colact, temb, proj, ot, xall, loads, ssem, rsem, xs, xr, lsem, taps):
    rows, cols, chan = at.rows, at.cols, at.chan
    tile = rows * cols
    add = lax.dot_general(ot[...], proj[3], (((0,), (0,)), ((), ())), preferred_element_type=F32)
    stats = zero_stats(chan)
    for m in range(at.seg):
        y = (xall[0, m * tile:(m + 1) * tile].astype(F32) + add[m * tile:(m + 1) * tile]).astype(BF16)
        xin[m * rows:(m + 1) * rows] = y.reshape(rows, cols, chan)
        vals = y.astype(F32)
        stats = add_stats(stats, vals)
        keep_cols(colbuf.at[2], m * rows, vals, rows, cols)
    swap_all(at, stats, mine.at[3], every.at[3], gather, ssem.at[3], rsem.at[3], xin, hrow.at[2], colbuf.at[2], hcol.at[2])
    conv_pair(at, count, 1, 3, 2, temb, norms, gather, spread, xin, hid, taps, wbuf, mine, every, hrow, colbuf, hcol, colact, loads[2:4], None, ssem, rsem)
    ybuf = hid

    def back(m):
        row = at.half * at.seg + m
        src = ybuf.at[pl.ds(m * rows, rows)]
        return row, pltpu.make_async_copy(src, y_out.at[at.img], lsem), remote(src, y_out.at[at.img], xs.at[m], xr.at[at.img], {'row': row, 'col': at.col})

    near_first = (1 - ((at.img + 1) // 2) % 2 + at.half) % 2

    def second(t, _):
        m = (t + near_first * (at.seg // 2)) % at.seg
        acc = conv_rows(at, taps, wbuf.at[1], m * rows)
        y = (xin[pl.ds(m * rows, rows)].astype(F32).reshape(tile, chan) + acc).astype(BF16)
        ybuf[pl.ds(m * rows, rows)] = y.reshape(rows, cols, chan)
        row, local, far = back(m)

        @pl.when(row == at.row)
        def _():
            local.start()

        @pl.when(row != at.row)
        def _():
            far.start()

        return 0

    lax.fori_loop(0, at.seg, second, 0)
    for m in range(at.seg):
        row, local, far = back(m)

        @pl.when(row == at.row)
        def _():
            local.wait()

        @pl.when(row != at.row)
        def _():
            far.wait_send()

    for i in range(at.n_img):
        row = i * at.halves + at.row // at.seg

        @pl.when(row != at.row)
        def _():
            remote(ybuf.at[pl.ds(0, rows)], y_out.at[i], xs.at[0], xr.at[i], {'row': row, 'col': at.col}).wait_recv()


def solution(mesh):
    n_row = mesh.shape['row']
    n_col = mesh.shape['col']

    def run_stage(latent, t_emb, res_norm, res_conv, res_temb, attn_norm, attn_proj):
        n_img, rows, cols, chan = latent.shape
        n_head, dim = attn_proj.shape[1], attn_proj.shape[3]
        dims = (n_img, n_row, n_col, rows, cols, chan)
        halves, seg = n_row // n_img, n_row // (n_row // n_img)
        n_peer = halves * n_col
        own = rows * seg
        tok = own * cols
        per_group = chan // GROUPS
        count = float(n_row * rows * n_col * cols * per_group)
        group_id = np.arange(chan) // per_group
        member = (group_id[:, None] == np.arange(128)[None, :]).astype(np.float32)
        proj = attn_proj.transpose(0, 1, 3, 2).reshape(4, n_head * dim, chan)
        n_msg = n_peer - 1 + 5
        n_stage = 5
        vmem, anywhere = pl.BlockSpec(memory_space=pltpu.VMEM), pl.BlockSpec(memory_space=pl.ANY)
        return pl.pallas_call(
            functools.partial(stage, dims, count, n_head),
            out_shape=jax.ShapeDtypeStruct(latent.shape, BF16),
            in_specs=[anywhere, vmem, anywhere, vmem, anywhere, vmem, anywhere, vmem, vmem],
            out_specs=anywhere,
            scratch_shapes=[
                pltpu.VMEM((own, cols, chan), BF16),
                pltpu.VMEM((own, cols, chan), BF16),
                pltpu.VMEM((2, 3, 3, chan, chan), BF16),
                pltpu.VMEM((n_stage, 8, 128), F32),
                pltpu.VMEM((n_stage, n_peer, 8, 128), F32),
                pltpu.VMEM((4, cols, chan), BF16),
                pltpu.VMEM((4, 2, own, chan), F32),
                pltpu.VMEM((4, 4, own, chan), F32),
                pltpu.VMEM((4, own, chan), F32),
                pltpu.VMEM((n_img, chan), F32),
                pltpu.VMEM(res_temb.shape[1:], BF16),
                pltpu.VMEM((4, n_head * dim, chan), BF16),
                pltpu.VMEM((n_head * dim, tok), BF16),
                pltpu.VMEM((4, tok, chan), BF16),
                pltpu.VMEM((4, 2 * tok, 2 * chan), BF16),
                pltpu.VMEM((4, chan, 2 * tok), BF16),
                pltpu.SemaphoreType.DMA((7,)),
                pltpu.SemaphoreType.DMA((n_stage, n_msg)),
                pltpu.SemaphoreType.DMA((n_stage, n_msg)),
                pltpu.SemaphoreType.DMA((n_img,)),
                pltpu.SemaphoreType.DMA((seg,)),
                pltpu.SemaphoreType.DMA((seg,)),
                pltpu.SemaphoreType.DMA((n_img,)),
                pltpu.SemaphoreType.DMA,
                pltpu.SemaphoreType.DMA((14,)),
                pltpu.SemaphoreType.DMA((14,)),
            ],
            compiler_params=pltpu.CompilerParams(collective_id=0, has_side_effects=True, vmem_limit_bytes=67043328),
            name='unet_stage',
        )(latent, t_emb, res_temb, res_norm, res_conv, attn_norm, proj, jnp.asarray(member, BF16), jnp.asarray(member.T.copy(), BF16))

    spec_x = P('dp', 'row', 'col', None)
    return jax.shard_map(run_stage, mesh=mesh, in_specs=(spec_x, P('dp', None), P(), P(), P(), P(), P()), out_specs=spec_x, check_vma=False)
```

```python
import functools

import jax
import jax.numpy as jnp
import numpy as np
from jax import lax
from jax.experimental import pallas as pl
from jax.experimental.pallas import tpu as pltpu
from jax.sharding import PartitionSpec as P

GROUPS = 32
EPS = 1e-5
F32 = jnp.float32
BF16 = jnp.bfloat16
LOG2E = 1.4426950408889634
KEY_BLK = 512
QUERY_TILE = 256
HEADS_PER_STEP = 5


class Place:
    def __init__(self, dims):
        self.n_img, self.n_row, self.n_col, self.rows, self.cols, self.chan = dims
        self.halves = self.n_row // self.n_img
        self.seg = self.n_row // self.halves
        self.row = lax.axis_index('row')
        self.col = lax.axis_index('col')
        self.img = self.row // self.halves
        self.half = self.row % self.halves
        self.n_peer = self.halves * self.n_col
        self.me = self.half * self.n_col + self.col

    def peer(self, step):
        slot = (self.me + step) % self.n_peer
        return {'row': self.img * self.halves + slot // self.n_col, 'col': slot % self.n_col}

    def partner(self):
        return {'row': self.img * self.halves + (1 - self.half), 'col': self.col}

    def beside(self, step, other=False):
        half = (1 - self.half) if other else self.half
        return {'row': self.img * self.halves + half, 'col': (self.col + step + self.n_col) % self.n_col}


def remote(src, dst, send_sem, recv_sem, device):
    return pltpu.make_async_remote_copy(src_ref=src, dst_ref=dst, send_sem=send_sem, recv_sem=recv_sem, device_id=device, device_id_type=pl.DeviceIdType.MESH)


def signal_peers(at, with_column):
    barrier = pltpu.get_barrier_semaphore()
    for step in range(1, at.n_peer):
        pl.semaphore_signal(barrier, inc=1, device_id=at.peer(step), device_id_type=pl.DeviceIdType.MESH)
    count = at.n_peer - 1
    if with_column:
        for step in range(1, at.n_img):
            for half in range(at.halves):
                row = ((at.img + step) % at.n_img) * at.halves + half
                pl.semaphore_signal(barrier, inc=1, device_id={'row': row, 'col': at.col}, device_id_type=pl.DeviceIdType.MESH)
                count += 1
    return count


def wait_peers(count):
    pl.semaphore_wait(pltpu.get_barrier_semaphore(), count)


def stat_copies(at, mine, every, ssem, rsem):
    out = []
    for step in range(1, at.n_peer):
        send = remote(mine, every.at[at.me], ssem.at[step - 1], rsem.at[step - 1], at.peer(step))
        source = (at.me - step + at.n_peer) % at.n_peer
        recv = remote(mine, every.at[source], ssem.at[step - 1], rsem.at[step - 1], at.peer(step))
        out.append((send, recv))
    return out


def halo_copies(at, full, hrow, colbuf, hcol, ssem, rsem):
    base = at.n_peer - 1
    edge = (at.rows * at.seg - 1) * (1 - at.half)
    out = []
    copy = remote(full.at[edge], hrow, ssem.at[base], rsem.at[base], at.partner())
    out.append((copy, copy))
    for slot, (side, step, other) in enumerate([(1, 1, False), (1, 1, True), (0, -1, False), (0, -1, True)]):
        copy = remote(colbuf.at[side], hcol.at[slot], ssem.at[base + 1 + slot], rsem.at[base + 1 + slot], at.beside(step, other))
        out.append((copy, copy))
    return out


def split_dot(vals, matrix):
    high = vals.astype(BF16).astype(F32)
    mid = (vals - high).astype(BF16).astype(F32)
    low = (vals - high - mid).astype(BF16).astype(F32)
    stacked = jnp.concatenate([high, mid, low, jnp.zeros_like(low)], axis=0).astype(BF16)
    out = jnp.dot(stacked, matrix, preferred_element_type=F32)
    return out[0:8] + out[8:16] + out[16:24]


def two_rows(first, second, shape):
    idx = lax.broadcasted_iota(jnp.int32, shape, 0)
    return jnp.where(idx == 0, first, jnp.where(idx == 1, second, 0.0))


def put_stats(stats, mine, every, gather, at):
    s1 = jnp.sum(stats[0], axis=0, keepdims=True)
    s2 = jnp.sum(stats[1], axis=0, keepdims=True)
    groups = split_dot(two_rows(s1, s2, stats[0].shape), gather[...])
    mine[...] = groups
    every[at.me] = groups


def swap_all(at, stats, mine, every, gather, ssem, rsem, full=None, hrow=None, colbuf=None, hcol=None, behind=()):
    halos = [] if full is None else halo_copies(at, full, hrow, colbuf, hcol, ssem, rsem)
    for send, _ in halos:
        send.start()
    put_stats(stats, mine, every, gather, at)
    sums = stat_copies(at, mine, every, ssem, rsem)
    for send, _ in sums:
        send.start()
    for copy in behind:
        copy.start()
    for _, recv in sums + halos:
        recv.wait_recv()
    for send, _ in sums + halos:
        send.wait_send()


def norm_terms(every, spread, scale, shift, count):
    total = every[0]
    for slot in range(1, every.shape[0]):
        total = total + every[slot]
    mean = total[0:1] / count
    inv = lax.rsqrt(total[1:2] / count - mean * mean + EPS)
    wide = split_dot(two_rows(mean, inv, total.shape), spread[...])
    return wide[0:1], wide[1:2] * scale, shift


def activate(x, terms):
    mean, scale, shift = terms
    half = ((x - mean) * scale + shift) * 0.5
    return half + half * jnp.tanh(half)


def add_stats(stats, vals):
    n, chan = vals.shape
    split = vals.reshape(n // 8, 8, chan)
    return stats[0] + jnp.sum(split, axis=0), stats[1] + jnp.sum(split * split, axis=0)


def zero_stats(chan):
    return jnp.zeros((8, chan), F32), jnp.zeros((8, chan), F32)


def keep_cols(colbuf, first_row, vals, n_rows, cols):
    for k in range(n_rows):
        colbuf[0, pl.ds(first_row + k, 1), :] = vals[k * cols:k * cols + 1]
        colbuf[1, pl.ds(first_row + k, 1), :] = vals[(k + 1) * cols - 1:(k + 1) * cols]


def fill_taps(at, full, hrow, hcol, terms, taps, colact):
    chan, cols = at.chan, at.cols
    n_own = at.rows * at.seg
    for slot in range(4):
        inside = (at.col > 0) if slot < 2 else (at.col < at.n_col - 1)
        colact[slot] = jnp.where(inside, activate(hcol[slot], terms), 0.0)
    row_id = lax.broadcasted_iota(jnp.int32, (cols, chan), 0)

    def put(dst, x, left, right):
        act = activate(x.astype(F32), terms)
        prev = jnp.where(row_id == 0, left, pltpu.roll(act, 1, 0))
        nxt = jnp.where(row_id == cols - 1, right, pltpu.roll(act, cols - 1, 0))
        taps[dst, :, 0:chan] = prev.astype(BF16)
        taps[dst, :, chan:2 * chan] = act.astype(BF16)
        taps[dst, :, 2 * chan:3 * chan] = nxt.astype(BF16)

    def own(r, _):
        put(r + 1, full[r], colact[0, pl.ds(r, 1), :], colact[2, pl.ds(r, 1), :])
        return 0

    lax.fori_loop(0, n_own, own, 0)
    near = (n_own - 1) * at.half
    put((n_own + 1) * (1 - at.half), hrow[...], colact[1, pl.ds(near, 1), :], colact[3, pl.ds(near, 1), :])
    taps[(n_own + 1) * at.half] = jnp.zeros((cols, 3 * chan), BF16)


def conv_rows(at, taps, weights, first):
    acc = None
    for dy in range(3):
        lhs = taps[pl.ds(first + dy, at.rows)].reshape(at.rows * at.cols, 3 * at.chan)
        part = jnp.dot(lhs, weights[dy].reshape(3 * at.chan, at.chan), preferred_element_type=F32)
        acc = part if acc is None else acc + part
    return acc


def norm_rows(ref):
    vals = ref[...].astype(F32)
    return vals[0:1], vals[1:2]


def spread_images(at, latent, xin, xs, xr, lsem, colbuf):
    target_half, slot = at.row // at.seg, at.row % at.seg
    rows, cols, chan = at.rows, at.cols, at.chan
    for i in range(at.n_img):
        row = i * at.halves + target_half
        dst = xin.at[pl.ds(slot * rows, rows)]

        @pl.when(row == at.row)
        def _():
            pltpu.make_async_copy(latent.at[i], dst, lsem).start()

        @pl.when(row != at.row)
        def _():
            remote(latent.at[i], dst, xs.at[i], xr.at[slot], {'row': row, 'col': at.col}).start()

    yield
    stats = zero_stats(chan)
    for k in range(at.seg):
        row = at.half * at.seg + k
        dst = xin.at[pl.ds(k * rows, rows)]

        @pl.when(row == at.row)
        def _():
            pltpu.make_async_copy(latent.at[0], dst, lsem).wait()

        @pl.when(row != at.row)
        def _():
            remote(latent.at[0], dst, xs.at[0], xr.at[k], {'row': row, 'col': at.col}).wait_recv()

        vals = xin[k * rows:(k + 1) * rows].astype(F32).reshape(rows * cols, chan)
        stats = add_stats(stats, vals)
        keep_cols(colbuf, k * rows, vals, rows, cols)
    yield stats
    for i in range(at.n_img):
        row = i * at.halves + target_half

        @pl.when(row != at.row)
        def _():
            remote(latent.at[i], xin.at[pl.ds(slot * rows, rows)], xs.at[i], xr.at[slot], {'row': row, 'col': at.col}).wait_send()

    yield


def conv_pair(at, count, blk, stage, halo, temb, norms, gather, spread, xin, hid, taps, wbuf, mine, every, hrow, colbuf, hcol, colact, loads, after_first, ssem, rsem):
    rows, cols, chan = at.rows, at.cols, at.chan
    terms = norm_terms(every.at[stage], spread, *norm_rows(norms.at[blk, 0]), count)
    fill_taps(at, xin, hrow.at[halo], hcol.at[halo], terms, taps, colact)
    loads[0].wait()
    shift = temb[blk, pl.ds(at.img, 1), :]

    def first(m, stats):
        h = (conv_rows(at, taps, wbuf.at[0], m * rows) + shift).astype(BF16)
        hid[pl.ds(m * rows, rows)] = h.reshape(rows, cols, chan)
        vals = h.astype(F32)
        keep_cols(colbuf.at[halo + 1], m * rows, vals, rows, cols)
        return add_stats(stats, vals)

    stats = lax.fori_loop(0, at.seg, first, zero_stats(chan))
    if after_first is not None:
        after_first.start()
    swap_all(at, stats, mine.at[stage + 1], every.at[stage + 1], gather, ssem.at[stage + 1], rsem.at[stage + 1], hid, hrow.at[halo + 1], colbuf.at[halo + 1], hcol.at[halo + 1])
    terms = norm_terms(every.at[stage + 1], spread, *norm_rows(norms.at[blk, 1]), count)
    fill_taps(at, hid, hrow.at[halo + 1], hcol.at[halo + 1], terms, taps, colact)
    loads[1].wait()


def time_terms(t_emb, weights, out):
    u = t_emb[...].astype(F32)
    act = (u / (1.0 + jnp.exp(-u))).astype(BF16)
    out[...] = jnp.dot(act, weights[...], preferred_element_type=F32)


def nt(a, b):
    return lax.dot_general(a, b, (((1,), (1,)), ((), ())), preferred_element_type=F32)


def gather_links(at, xall, ssem, rsem):
    half_tok = xall.shape[1] // 2
    right, left = at.beside(1), at.beside(-1)
    low, high = pl.ds(0, half_tok), pl.ds(half_tok, half_tok)
    x = xall.at[0]
    ends = [(x.at[low], xall.at[1, low], right), (x.at[high], xall.at[2, low], right), (x.at[high], xall.at[1, high], left), (x.at[low], xall.at[2, high], left), (xall.at[1, low], xall.at[3, low], right), (xall.at[1, high], xall.at[3, high], left)]
    return [remote(src, dst, ssem.at[k], rsem.at[k], device) for k, (src, dst, device) in enumerate(ends)]


def attention(at, count, every, norms, spread, proj, load, out, xall, kbuf, vbuf, ssem, rsem, qm, sbuf, run_max, run_sum, run_out):
    _, tok, chan = xall.shape
    n_head = qm.shape[0]
    dim = chan // n_head
    x = xall.at[0]
    terms = norm_terms(every, spread, *norm_rows(norms), count)
    mate = at.partner()

    def link(k, src, slot, device):
        return remote(src, slot, ssem.at[k], rsem.at[k], device)

    low_right, high_right, high_left, low_left, far_low, far_high = gather_links(at, xall, ssem, rsem)
    second = pl.ds(tok, tok)

    def keys_over(k):
        return link(6 + k, kbuf.at[k, pl.ds(0, tok)], kbuf.at[k, second], mate)

    def values_over(k):
        return link(10 + k, vbuf.at[k, :, pl.ds(0, tok)], vbuf.at[k, :, second], mate)

    load.wait()
    first_half = lax.broadcasted_iota(jnp.int32, (tok, 2 * dim), 1) < dim

    def normed(vals):
        return ((vals.astype(F32) - terms[0]) * terms[1] + terms[2]).astype(BF16)

    def project(k, _):
        @pl.when(k == 1)
        def _():
            low_right.wait_recv()
            far_low.start()
            high_left.wait_recv()
            far_high.start()

        @pl.when(k == 2)
        def _():
            high_right.wait_recv()
            low_left.wait_recv()

        @pl.when(k == 3)
        def _():
            far_low.wait_recv()
            far_high.wait_recv()

        g = normed(xall[k])
        keys = nt(g, proj[1])
        for p in range(n_head // 2):
            both = keys[:, p * 2 * dim:(p + 1) * 2 * dim]
            swapped = pltpu.roll(both, dim, 1)
            kbuf[k, 0:tok, 4 * p * dim:(4 * p + 2) * dim] = jnp.where(first_half, both, swapped).astype(BF16)
            kbuf[k, 0:tok, (4 * p + 2) * dim:(4 * p + 4) * dim] = jnp.where(first_half, swapped, both).astype(BF16)
        vbuf[k, :, 0:tok] = nt(proj[2], g).astype(BF16)
        keys_over(k).start()
        values_over(k).start()
        return 0

    def queries():
        run_max[...] = jnp.full(run_max.shape, -1e30, F32)
        run_sum[...] = jnp.zeros(run_sum.shape, F32)
        run_out[...] = jnp.zeros(run_out.shape, F32)
        qt = nt(proj[0], normed(x[...])).astype(BF16).astype(F32) * (LOG2E * dim ** -0.5)
        hi = qt.astype(BF16)
        rest = qt - hi.astype(F32)
        mid = rest.astype(BF16)
        lo = (rest - mid.astype(F32)).astype(BF16)
        for h in range(n_head):
            rows = slice(h * dim, (h + 1) * dim)
            qm[h, 0:dim, :] = hi[rows]
            qm[h, dim:2 * dim, :] = mid[rows]
            qm[h, 2 * dim:3 * dim, :] = lo[rows]
            qm[h, 3 * dim:4 * dim, :] = jnp.zeros((dim, tok), BF16)

    n_blk = 2 * tok // KEY_BLK
    n_slot = sbuf.shape[0]
    assert HEADS_PER_STEP * n_blk % n_slot == 0

    def attend(k, _):
        keys_over(k).wait_recv()
        values_over(k).wait_recv()

        def produce(h, j, slot, cols):
            keys = kbuf[k, pl.ds(j * KEY_BLK, KEY_BLK), pl.ds(pl.multiple_of(h * 2 * dim, 2 * dim), 2 * dim)]
            s = jnp.dot(jnp.concatenate([keys, keys], axis=1), qm[h, :, cols], preferred_element_type=F32)
            sbuf[slot, :, cols] = s
            return jnp.max(s.reshape(KEY_BLK // 8, 8, QUERY_TILE), axis=0)

        tiles = [slice(q, q + QUERY_TILE) for q in range(0, tok, QUERY_TILE)]

        def heads(p, tops):
            for u in range(HEADS_PER_STEP * n_blk):
                h, j = HEADS_PER_STEP * p + u // n_blk, u % n_blk
                nh, nj = HEADS_PER_STEP * p + (u + 1) // n_blk, (u + 1) % n_blk
                if u + 1 == HEADS_PER_STEP * n_blk:
                    nh = jnp.minimum(nh, n_head - 1)
                ahead = []
                for q, cols in enumerate(tiles):
                    ahead.append(produce(nh, nj, (u + 1) % n_slot, cols))
                    m, l, acc = run_max[h, 0:1, cols], run_sum[h, :, cols], run_out[h, :, cols]
                    new = jnp.maximum(m, jnp.max(tops[q], axis=0, keepdims=True))
                    alpha = jnp.exp2(m - new)
                    w = jnp.exp2(sbuf[u % n_slot, :, cols] - new)
                    run_sum[h, :, cols] = l * alpha + jnp.sum(w.reshape(KEY_BLK // 8, 8, QUERY_TILE), axis=0)
                    run_max[h, 0:1, cols] = new
                    vt = vbuf[k, pl.ds(pl.multiple_of(h * dim, dim), dim), j * KEY_BLK:(j + 1) * KEY_BLK]
                    run_out[h, :, cols] = acc * alpha + jnp.dot(vt, w.astype(BF16), preferred_element_type=F32)
                tops = ahead

            @pl.when(jnp.logical_and(p == 0, k < 3))
            def _():
                project(k + 1, 0)

            return tuple(tops)

        lax.fori_loop(0, n_head // HEADS_PER_STEP, heads, tuple(produce(0, 0, 0, cols) for cols in tiles))
        return 0

    project(0, 0)
    queries()
    lax.fori_loop(0, 4, attend, 0)
    for copy in (low_right, high_right, high_left, low_left, far_low, far_high):
        copy.wait_send()
    for k in range(4):
        keys_over(k).wait_send()
        values_over(k).wait_send()

    def finish(h, _):
        total = jnp.sum(run_sum[h], axis=0, keepdims=True)
        out[pl.ds(pl.multiple_of(h * dim, dim), dim), :] = (run_out[h] / total).astype(BF16)
        return 0

    lax.fori_loop(0, n_head, finish, 0)


def stage(dims, count, n_head, latent, t_emb_in, w_temb, norms_in, w_all, a_norms_in, proj_all, gather_in, spread_in, y_out, t_emb, norms, a_norms, gather, spread, xin, wbuf, mine, every, hrow, colbuf, hcol, colact, temb, proj, xall, kbuf, vbuf, wsem, ssem, rsem, xs, xr, ys, yr, lsem, asend, arecv):
    at = Place(dims)
    n_wait = signal_peers(at, True)
    rows, cols, chan = at.rows, at.cols, at.chan
    tile = rows * cols
    tok = tile * at.seg
    ot = vbuf.at[0, :, pl.ds(0, tok)]
    loads = [pltpu.make_async_copy(w_all.at[blk, j], wbuf.at[j], wsem.at[2 * blk + j]) for blk in range(2) for j in range(2)]
    proj_load = pltpu.make_async_copy(proj_all, proj, wsem.at[6])
    small = ((t_emb_in, t_emb), (norms_in, norms), (a_norms_in, a_norms), (gather_in, gather), (spread_in, spread))
    small_loads = [pltpu.make_async_copy(src, dst, wsem.at[7 + i]) for i, (src, dst) in enumerate(small)]
    for load in small_loads:
        load.start()
    wait_peers(n_wait)
    images = spread_images(at, latent, xin, xs, xr, lsem, colbuf.at[0])
    next(images)
    loads[0].start()
    loads[1].start()
    proj_load.start()
    for load in small_loads:
        load.wait()

    def times(tbuf):
        copies = [pltpu.make_async_copy(w_temb.at[blk], tbuf.at[blk], wsem.at[4 + blk]) for blk in range(2)]
        for copy in copies:
            copy.start()
        for blk, copy in enumerate(copies):
            copy.wait()
            time_terms(t_emb, tbuf.at[blk], temb.at[blk])

    pl.run_scoped(times, pltpu.VMEM(w_temb.shape, BF16))
    stats = next(images)
    swap_all(at, stats, mine.at[0], every.at[0], gather, ssem.at[0], rsem.at[0], xin, hrow.at[0], colbuf.at[0], hcol.at[0])
    next(images)
    conv_bufs = pltpu.VMEM((rows * at.seg + 2, cols, 3 * chan), BF16), pltpu.VMEM(xin.shape, BF16)

    def first_block(taps, hid):
        conv_pair(at, count, 0, 0, 0, temb, norms, gather, spread, xin, hid, taps, wbuf, mine, every, hrow, colbuf, hcol, colact, loads[0:2], loads[2], ssem, rsem)

        def second(m, stats):
            acc = conv_rows(at, taps, wbuf.at[1], m * rows)
            y = (xin[pl.ds(m * rows, rows)].astype(F32).reshape(tile, chan) + acc).astype(BF16)
            xall[0, pl.ds(m * tile, tile)] = y
            return add_stats(stats, y.astype(F32))

        stats = lax.fori_loop(0, at.seg, second, zero_stats(chan))
        loads[3].start()
        links = gather_links(at, xall, asend, arecv)
        swap_all(at, stats, mine.at[2], every.at[2], gather, ssem.at[2], rsem.at[2], behind=(links[0], links[2], links[1], links[3]))

    pl.run_scoped(first_block, *conv_bufs)

    dim = chan // n_head
    pl.run_scoped(
        functools.partial(attention, at, count, every.at[2], a_norms, spread, proj, proj_load, ot, xall, kbuf, vbuf, asend, arecv),
        pltpu.VMEM((n_head, 4 * dim, tok), BF16),
        pltpu.VMEM((3, KEY_BLK, tok), F32),
        pltpu.VMEM((n_head, 8, tok), F32),
        pltpu.VMEM((n_head, 8, tok), F32),
        pltpu.VMEM((n_head, dim, tok), F32),
    )
    pl.run_scoped(functools.partial(second_block, at, count, norms, gather, spread, y_out, xin, wbuf, mine, every, hrow, colbuf, hcol, colact, temb, proj, ot, xall, loads, ssem, rsem, ys, yr, lsem), *conv_bufs)


def second_block(at, count, norms, gather, spread, y_out, xin, wbuf, mine, every, hrow, colbuf, hcol, colact, temb, proj, ot, xall, loads, ssem, rsem, xs, xr, lsem, taps, hid):
    rows, cols, chan = at.rows, at.cols, at.chan
    tile = rows * cols
    add = lax.dot_general(ot[...], proj[3], (((0,), (0,)), ((), ())), preferred_element_type=F32)
    stats = zero_stats(chan)
    for m in range(at.seg):
        y = (xall[0, m * tile:(m + 1) * tile].astype(F32) + add[m * tile:(m + 1) * tile]).astype(BF16)
        xin[m * rows:(m + 1) * rows] = y.reshape(rows, cols, chan)
        vals = y.astype(F32)
        stats = add_stats(stats, vals)
        keep_cols(colbuf.at[2], m * rows, vals, rows, cols)
    swap_all(at, stats, mine.at[3], every.at[3], gather, ssem.at[3], rsem.at[3], xin, hrow.at[2], colbuf.at[2], hcol.at[2])
    conv_pair(at, count, 1, 3, 2, temb, norms, gather, spread, xin, hid, taps, wbuf, mine, every, hrow, colbuf, hcol, colact, loads[2:4], None, ssem, rsem)
    ybuf = hid

    def back(m):
        row = at.half * at.seg + m
        src = ybuf.at[pl.ds(m * rows, rows)]
        return row, pltpu.make_async_copy(src, y_out.at[at.img], lsem), remote(src, y_out.at[at.img], xs.at[m], xr.at[at.img], {'row': row, 'col': at.col})

    near_first = (1 - ((at.img + 1) // 2) % 2 + at.half) % 2

    def second(t, _):
        m = (t + near_first * (at.seg // 2)) % at.seg
        acc = conv_rows(at, taps, wbuf.at[1], m * rows)
        y = (xin[pl.ds(m * rows, rows)].astype(F32).reshape(tile, chan) + acc).astype(BF16)
        ybuf[pl.ds(m * rows, rows)] = y.reshape(rows, cols, chan)
        row, local, far = back(m)

        @pl.when(row == at.row)
        def _():
            local.start()

        @pl.when(row != at.row)
        def _():
            far.start()

        return 0

    lax.fori_loop(0, at.seg, second, 0)
    for m in range(at.seg):
        row, local, far = back(m)

        @pl.when(row == at.row)
        def _():
            local.wait()

        @pl.when(row != at.row)
        def _():
            far.wait_send()

    for i in range(at.n_img):
        row = i * at.halves + at.row // at.seg

        @pl.when(row != at.row)
        def _():
            remote(ybuf.at[pl.ds(0, rows)], y_out.at[i], xs.at[0], xr.at[i], {'row': row, 'col': at.col}).wait_recv()


def solution(mesh):
    n_row = mesh.shape['row']
    n_col = mesh.shape['col']

    def run_stage(latent, t_emb, res_norm, res_conv, res_temb, attn_norm, attn_proj):
        n_img, rows, cols, chan = latent.shape
        n_head, dim = attn_proj.shape[1], attn_proj.shape[3]
        dims = (n_img, n_row, n_col, rows, cols, chan)
        halves, seg = n_row // n_img, n_row // (n_row // n_img)
        n_peer = halves * n_col
        own = rows * seg
        tok = own * cols
        per_group = chan // GROUPS
        count = float(n_row * rows * n_col * cols * per_group)
        group_id = np.arange(chan) // per_group
        member = (group_id[:, None] == np.arange(128)[None, :]).astype(np.float32)
        proj = attn_proj.transpose(0, 1, 3, 2).reshape(4, n_head * dim, chan)
        n_msg = n_peer - 1 + 5
        n_stage = 5
        anywhere = pl.BlockSpec(memory_space=pl.ANY)
        return pl.pallas_call(
            functools.partial(stage, dims, count, n_head),
            out_shape=jax.ShapeDtypeStruct(latent.shape, BF16),
            in_specs=[anywhere] * 9,
            out_specs=anywhere,
            scratch_shapes=[
                pltpu.VMEM(t_emb.shape, BF16),
                pltpu.VMEM(res_norm.shape, BF16),
                pltpu.VMEM(attn_norm.shape, BF16),
                pltpu.VMEM((chan, 128), BF16),
                pltpu.VMEM((128, chan), BF16),
                pltpu.VMEM((own, cols, chan), BF16),
                pltpu.VMEM((2, 3, 3, chan, chan), BF16),
                pltpu.VMEM((n_stage, 8, 128), F32),
                pltpu.VMEM((n_stage, n_peer, 8, 128), F32),
                pltpu.VMEM((4, cols, chan), BF16),
                pltpu.VMEM((4, 2, own, chan), F32),
                pltpu.VMEM((4, 4, own, chan), F32),
                pltpu.VMEM((4, own, chan), F32),
                pltpu.VMEM((2, n_img, chan), F32),
                pltpu.VMEM((4, n_head * dim, chan), BF16),
                pltpu.VMEM((4, tok, chan), BF16),
                pltpu.VMEM((4, 2 * tok, 2 * chan), BF16),
                pltpu.VMEM((4, chan, 2 * tok), BF16),
                pltpu.SemaphoreType.DMA((12,)),
                pltpu.SemaphoreType.DMA((n_stage, n_msg)),
                pltpu.SemaphoreType.DMA((n_stage, n_msg)),
                pltpu.SemaphoreType.DMA((n_img,)),
                pltpu.SemaphoreType.DMA((seg,)),
                pltpu.SemaphoreType.DMA((seg,)),
                pltpu.SemaphoreType.DMA((n_img,)),
                pltpu.SemaphoreType.DMA,
                pltpu.SemaphoreType.DMA((14,)),
                pltpu.SemaphoreType.DMA((14,)),
            ],
            compiler_params=pltpu.CompilerParams(collective_id=0, has_side_effects=True, vmem_limit_bytes=67043328),
            name='unet_stage',
        )(latent, t_emb, res_temb, res_norm, res_conv, attn_norm, proj, jnp.asarray(member, BF16), jnp.asarray(member.T.copy(), BF16))

    spec_x = P('dp', 'row', 'col', None)
    return jax.shard_map(run_stage, mesh=mesh, in_specs=(spec_x, P('dp', None), P(), P(), P(), P(), P()), out_specs=spec_x, check_vma=False)
```
